32 devices in a mesh: dp: 2 (over x), tp: 4 (over z), sp: 4 (over y, core).
Axes of the slice: x: 2, y: 2, z: 4, core: 2. Of those that a mesh axis runs over, the one named last changes fastest.
Arguments:
- x_in: bfloat16 [32, 4096, 1024], P('dp', ('tp', 'sp')), parts along dimension 0
- q_out: bfloat16 [32, 4096, 1024], P('dp', ('tp', 'sp')), parts along dimension 0
- latents: bfloat16 [64, 1024], replicated
- norm_in: float32 [2, 1024], replicated
- norm_query: float32 [2, 1024], replicated
- norm_lat: float32 [8, 2, 1024], replicated
- enc_wq: bfloat16 [1024, 1024], replicated
- enc_wkv: bfloat16 [2, 1024, 1024], replicated
- enc_wo: bfloat16 [1024, 1024], replicated
- enc_mlp: bfloat16 [2, 1024, 1024], replicated
- lat_wqkv: bfloat16 [2, 1024, 3, 8, 128], P(None, None, None, 'tp')
- lat_wo: bfloat16 [2, 8, 128, 1024], P(None, 'tp')
- lat_w1: bfloat16 [2, 1024, 4096], P(None, None, 'tp')
- lat_w2: bfloat16 [2, 4096, 1024], P(None, 'tp')
- dec_wq: bfloat16 [1024, 1024], replicated
- dec_wkv: bfloat16 [2, 1024, 1024], replicated
- dec_wo: bfloat16 [1024, 1024], replicated
- dec_mlp: bfloat16 [2, 1024, 1024], replicated
- dec_out: bfloat16 [1024, 1024], replicated
Outputs:
- output: float32 [32, 4096, 1024], P('dp', ('tp', 'sp')), parts along dimension 0
There are 2 independent parts. The reference program is written for one: setup_inputs(seed, part) draws one part's arguments, and reference() takes and returns one part's arrays. A program takes and returns all parts, laid end to end along the dimension named above; an argument that names none is the same for every part.
All inputs are finite; a program needn't handle non-finite values.
Results may differ from the reference program's by a relative error of at most 0.0104939.
Values sent between devices are 32-bit elements.
A program may use at most 1 GiB of HBM per device.

```python
import math
import jax
import jax.numpy as jnp
from jax import lax

BATCH = 16
M = 4096
N = 64
D = 1024
HEADS = 8
FF = 4096
C = 1024
CQ = 1024
CO = 1024

HEAD_DIM = D // HEADS
LN_EPS = 1e-5
ENC_SHARP = math.sqrt(math.log(M / 32.0))
LAT_SHARP = math.sqrt(math.log(N / 8.0))


def draw_normal(rng_key, arr_shape, std_scale):
    return (jax.random.normal(rng_key, arr_shape, jnp.float32) * std_scale).astype(jnp.bfloat16)


def draw_norms(rng_key, num_norms, feat_width):
    gain_key, bias_key = jax.random.split(rng_key)
    gain_rows = 1.0 + 0.25 * jax.random.normal(gain_key, (num_norms, 1, feat_width), jnp.float32)
    biases = 0.25 * jax.random.normal(bias_key, (num_norms, 1, feat_width), jnp.float32)
    return jnp.concatenate([gain_rows, biases], axis=1)


def setup_inputs(seed: int = 0, part: int = 0) -> dict:
    part_key = jax.random.fold_in(jax.random.key(seed), part)
    data_x, data_q = jax.random.split(part_key)
    shared = jax.random.split(jax.random.key(seed + 1), 17)
    qkv_scale = jnp.array([LAT_SHARP, 1.0, 1.0], jnp.float32).reshape(1, 1, 3, 1, 1) / math.sqrt(D)
    lat_wqkv = (jax.random.normal(shared[10], (2, D, 3, HEADS, HEAD_DIM), jnp.float32) * qkv_scale).astype(jnp.bfloat16)
    return {
        'x_in': draw_normal(data_x, (BATCH, M, C), 1.0),
        'q_out': draw_normal(data_q, (BATCH, M, CQ), 1.0),
        'latents': draw_normal(shared[0], (N, D), 1.0),
        'norm_in': draw_norms(shared[1], 1, C)[0],
        'norm_query': draw_norms(shared[2], 1, CQ)[0],
        'norm_lat': draw_norms(shared[3], 8, D),
        'enc_wq': draw_normal(shared[4], (D, D), ENC_SHARP / math.sqrt(D)),
        'enc_wkv': draw_normal(shared[5], (2, C, D), 1.0 / math.sqrt(C)),
        'enc_wo': draw_normal(shared[6], (D, D), 4.0 / math.sqrt(D)),
        'enc_mlp': draw_normal(shared[7], (2, D, D), 1.0 / math.sqrt(D)),
        'lat_wqkv': lat_wqkv,
        'lat_wo': draw_normal(shared[8], (2, HEADS, HEAD_DIM, D), 1.7 / math.sqrt(D)),
        'lat_w1': draw_normal(shared[9], (2, D, FF), 1.0 / math.sqrt(D)),
        'lat_w2': draw_normal(shared[11], (2, FF, D), 1.0 / math.sqrt(FF)),
        'dec_wq': draw_normal(shared[12], (CQ, D), LAT_SHARP / math.sqrt(CQ)),
        'dec_wkv': draw_normal(shared[13], (2, D, D), 1.0 / math.sqrt(D)),
        'dec_wo': draw_normal(shared[14], (D, D), 2.0 / math.sqrt(D)),
        'dec_mlp': draw_normal(shared[15], (2, D, D), 1.0 / math.sqrt(D)),
        'dec_out': draw_normal(shared[16], (D, CO), 1.0 / math.sqrt(D)),
    }


def layer_norm(values, params):
    val_f32 = values.astype(jnp.float32)
    row_mean = jnp.mean(val_f32, axis=-1, keepdims=True)
    centered = val_f32 - row_mean
    row_var = jnp.mean(centered * centered, axis=-1, keepdims=True)
    return (centered * lax.rsqrt(row_var + LN_EPS) * params[0] + params[1]).astype(jnp.bfloat16)


def mlp_block(residual, norm_params, w_up, w_down):
    hidden = jax.nn.gelu(jnp.dot(layer_norm(residual, norm_params), w_up, preferred_element_type=jnp.float32))
    return residual + jnp.dot(hidden.astype(jnp.bfloat16), w_down, preferred_element_type=jnp.float32)


def latent_layer(latent, layer_args):
    w_qkv, w_out, w_up, w_down, layer_norms = layer_args
    qkv_proj = jnp.dot(layer_norm(latent, layer_norms[0]), w_qkv.reshape(D, 3 * D), preferred_element_type=jnp.float32)
    qkv_proj = qkv_proj.astype(jnp.bfloat16).astype(jnp.float32).reshape(N, 3, HEADS, HEAD_DIM)
    att_scores = jnp.einsum('nhe,mhe->hnm', qkv_proj[:, 0], qkv_proj[:, 1]) / math.sqrt(HEAD_DIM)
    att_probs = jax.nn.softmax(att_scores, axis=-1).astype(jnp.bfloat16).astype(jnp.float32)
    att_out = jnp.einsum('hnm,mhe->nhe', att_probs, qkv_proj[:, 2]).astype(jnp.bfloat16).reshape(N, D)
    latent = latent + jnp.dot(att_out, w_out.reshape(D, D), preferred_element_type=jnp.float32)
    return mlp_block(latent, layer_norms[1], w_up, w_down), None


def reference(x_in, q_out, latents, norm_in, norm_query, norm_lat, enc_wq, enc_wkv, enc_wo, enc_mlp,
              lat_wqkv, lat_wo, lat_w1, lat_w2, dec_wq, dec_wkv, dec_wo, dec_mlp, dec_out):
    query_enc = jnp.dot(layer_norm(latents, norm_lat[0]), enc_wq, preferred_element_type=jnp.float32).astype(jnp.bfloat16)
    layer_stack = (lat_wqkv, lat_wo, lat_w1, lat_w2, norm_lat[2:6].reshape(2, 2, 2, D))

    def one_sequence(seq_pair):
        x_seq, q_seq = seq_pair
        normed_x = layer_norm(x_seq, norm_in)
        key_enc = jnp.dot(normed_x, enc_wkv[0], preferred_element_type=jnp.float32).astype(jnp.bfloat16)
        val_enc = jnp.dot(normed_x, enc_wkv[1], preferred_element_type=jnp.float32).astype(jnp.bfloat16)
        scores = jnp.dot(query_enc, key_enc.T, preferred_element_type=jnp.float32) / math.sqrt(D)
        weights = jnp.exp(scores - jnp.max(scores, axis=1, keepdims=True))
        numerator = jnp.dot(weights.astype(jnp.bfloat16), val_enc, preferred_element_type=jnp.float32)
        attended = (numerator / jnp.sum(weights, axis=1, keepdims=True)).astype(jnp.bfloat16)
        latent = latents.astype(jnp.float32) + jnp.dot(attended, enc_wo, preferred_element_type=jnp.float32)
        latent = mlp_block(latent, norm_lat[1], enc_mlp[0], enc_mlp[1])
        latent = lax.scan(latent_layer, latent, layer_stack)[0]
        normed_z = layer_norm(latent, norm_lat[6])
        key_dec = jnp.dot(normed_z, dec_wkv[0], preferred_element_type=jnp.float32).astype(jnp.bfloat16)
        val_dec = jnp.dot(normed_z, dec_wkv[1], preferred_element_type=jnp.float32).astype(jnp.bfloat16)
        query_dec = jnp.dot(layer_norm(q_seq, norm_query), dec_wq, preferred_element_type=jnp.float32).astype(jnp.bfloat16)
        dec_scores = jnp.dot(query_dec, key_dec.T, preferred_element_type=jnp.float32) / math.sqrt(D)
        dec_probs = jax.nn.softmax(dec_scores, axis=-1).astype(jnp.bfloat16)
        attended = jnp.dot(dec_probs, val_dec, preferred_element_type=jnp.float32).astype(jnp.bfloat16)
        output = jnp.dot(attended, dec_wo, preferred_element_type=jnp.float32)
        output = mlp_block(output, norm_lat[7], dec_mlp[0], dec_mlp[1])
        return jnp.dot(output.astype(jnp.bfloat16), dec_out, preferred_element_type=jnp.float32)

    return lax.map(one_sequence, (x_in, q_out))
```

```python
import functools
import math
import jax
import jax.numpy as jnp
from jax import lax
from jax.experimental import pallas as pl
from jax.experimental.pallas import tpu as pltpu
from jax.sharding import PartitionSpec as P

LN_EPS = 1e-5
F32, BF16 = jnp.float32, jnp.bfloat16
MESH = pl.DeviceIdType.MESH
VMEM_LIMIT = 60 * 1024 * 1024
LANES = 128
NLINE = 4
NCH = 4
GELU_C = math.sqrt(2.0 / math.pi)


def layer_norm(values, gain, bias):
    row_mean = jnp.mean(values, axis=-1, keepdims=True)
    centered = values - row_mean
    row_var = jnp.mean(centered * centered, axis=-1, keepdims=True)
    return (centered * lax.rsqrt(row_var + LN_EPS) * gain + bias).astype(BF16)


def gelu(x):
    return 0.5 * x * (1.0 + jnp.tanh(GELU_C * (x + 0.044715 * (x * x * x))))


def dot(a, b):
    return jnp.dot(a, b, preferred_element_type=F32)


def dot_t(a, b):
    return lax.dot_general(a, b, (((1,), (1,)), ((), ())), preferred_element_type=F32)


def split_bf16(x):
    high = x.astype(BF16)
    return high, (x - high.astype(F32)).astype(BF16)


def encoder_kernel(x_ref, nin_ref, lat_ref, nq_ref, wq_ref, wk_ref, num_ref, st_ref, qk_s, stats_s):
    b = pl.program_id(0)
    n = lat_ref.shape[0]
    dim = lat_ref.shape[1]

    @pl.when(b == 0)
    def _():
        q = dot(layer_norm(lat_ref[...].astype(F32), nq_ref[0:1, :], nq_ref[1:2, :]), wq_ref[...]).astype(BF16)
        high, low = split_bf16(dot_t(q, wk_ref[0]))
        qk_s[0:n, :] = high
        qk_s[n:2 * n, :] = low
        stats_s[...] = jnp.zeros_like(stats_s)

    xn = layer_norm(x_ref[0].astype(F32), nin_ref[0:1, :], nin_ref[1:2, :])
    both = dot_t(qk_s[...], xn)
    scores = (both[:n] + both[n:]) * (1.0 / math.sqrt(dim))
    row_max = jnp.max(scores, axis=1, keepdims=True)
    weights = jnp.exp(scores - row_max)
    row_sum = jnp.sum(weights, axis=1, keepdims=True)
    num_ref[0] = dot(weights.astype(BF16), xn)
    here = lax.broadcasted_iota(jnp.int32, (n, LANES), 1) == b
    stats_s[0:n, :] = jnp.where(here, row_max, stats_s[0:n, :])
    stats_s[n:2 * n, :] = jnp.where(here, row_sum, stats_s[n:2 * n, :])

    @pl.when(b == pl.num_programs(0) - 1)
    def _():
        st_ref[...] = stats_s[...].T[0:st_ref.shape[0], :]


def encoder_local(x_loc, norm_in, latents, norm_q, enc_wq, enc_wkv):
    nb, rows, dim = x_loc.shape
    n = latents.shape[0]
    whole = lambda shape: pl.BlockSpec(shape, lambda b: (0,) * len(shape))
    return pl.pallas_call(
        encoder_kernel,
        grid=(nb,),
        in_specs=[pl.BlockSpec((1, rows, dim), lambda b: (b, 0, 0)), whole((2, dim)), whole((n, dim)), whole((2, dim)),
                  whole((dim, dim)), pl.BlockSpec((1, dim, dim), lambda b: (0, 0, 0))],
        out_specs=[pl.BlockSpec((1, n, dim), lambda b: (b, 0, 0)), whole((nb, LANES))],
        out_shape=[jax.ShapeDtypeStruct((nb, n, dim), F32), jax.ShapeDtypeStruct((nb, LANES), F32)],
        scratch_shapes=[pltpu.VMEM((2 * n, dim), BF16), pltpu.VMEM((LANES, LANES), F32)],
        compiler_params=pltpu.CompilerParams(vmem_limit_bytes=VMEM_LIMIT),
        name='enc_local',
    )(x_loc, norm_in, latents, norm_q, enc_wq, enc_wkv)


def latent_kernel(num_ref, st_ref, lat_ref, nlat_ref, wkv_h, wo_h, emlp_h, qkv_h, lwo_h, lw1_h, lw2_h, out_ref,
                  wv, wo, emlp, wqkv, lwo, lw1, lw2, wsem,
                  st_all, gs, d2d, ysend, yrecv, zsum, rz_a, rz_b, ln_n, ln_f, ac_n, ac_f, zown, zall,
                  s_st, r_st, s_d2, r_d2, s_y, r_y, s_za, s_zb, r_za, r_zb,
                  s_lnn, s_lnf, s_acn, s_acf, r_lnn, r_lnf, r_acn, r_acf, r_ag, s_agz, s_agc, s_agy):
    n, dim = lat_ref.shape
    rows = n // NCH
    x = lax.axis_index('dp')
    t = lax.axis_index('tp')
    sp = lax.axis_index('sp')
    y = lax.div(sp, 2)
    c = lax.rem(sp, 2)
    me = t * 4 + sp
    upper = lax.div(t, 2)
    is_end = jnp.logical_or(t == 0, t == NLINE - 1)
    is_mid = jnp.logical_not(is_end)
    e_near = upper
    e_far = 1 - upper
    inward = (x, jnp.where(t == 0, 1, jnp.where(t == 1, 2, jnp.where(t == 2, 1, 2))), sp)
    outward = (x, jnp.where(t <= 1, 0, NLINE - 1), sp)
    core_peer = (x, t, y * 2 + (1 - c))
    y_peer = (x, t, (1 - y) * 2 + c)

    def rc(src, dst, ssem, rsem, dev):
        return pltpu.make_async_remote_copy(src_ref=src, dst_ref=dst, send_sem=ssem, recv_sem=rsem,
                                            device_id=dev, device_id_type=MESH)

    def peer(p):
        g = lax.rem(me + p, 16)
        return g, (x, lax.div(g, 4), lax.rem(g, 4))

    loads = [pltpu.make_async_copy(src, dst, wsem.at[i]) for i, (src, dst) in enumerate(
        ((wkv_h.at[1], wv), (wo_h, wo), (emlp_h, emlp), (qkv_h, wqkv), (lwo_h, lwo), (lw1_h, lw1), (lw2_h, lw2)))]
    for load in loads:
        load.start()

    barrier = pltpu.get_barrier_semaphore()

    def greet(p, carry):
        pl.semaphore_signal(barrier, inc=1, device_id=peer(p)[1], device_id_type=MESH)
        return carry

    lax.fori_loop(1, 16, greet, 0)
    pl.semaphore_wait(barrier, 15)

    def send_stats(p, carry):
        g, dev = peer(p)
        rc(st_ref, st_all.at[me], s_st.at[g], r_st.at[me], dev).start()
        return carry

    lax.fori_loop(1, 16, send_stats, 0)

    def core_copy(i, yb):
        return rc(num_ref.at[pl.ds(yb * 8 + (1 - c) * 4 + i * 2, 2)], d2d.at[i, yb], s_d2.at[i, yb], r_d2.at[i, yb], core_peer)

    for i in range(2):
        core_copy(i, 1 - y).start()
        core_copy(i, y).start()
    st_all[me] = st_ref[...]

    def wait_stats(p, carry):
        g, dev = peer(p)
        rc(st_ref, st_all.at[g], s_st.at[g], r_st.at[g], dev).wait_recv()
        return carry

    lax.fori_loop(1, 16, wait_stats, 0)
    top = lax.fori_loop(1, 16, lambda d, m: jnp.maximum(m, st_all[d]), st_all[0])

    def add_sum(d, total):
        stats = st_all[d]
        return total + jnp.exp(stats - top) * pltpu.roll(stats, n, 1)

    total = lax.fori_loop(0, 16, add_sum, jnp.zeros_like(top))
    partner = t * 4 + y * 2 + (1 - c)
    gs[...] = jnp.zeros_like(gs)
    gs[0:16, :] = jnp.exp(st_all[me] - top) / total
    scale_own = gs[...].T[0:n, :]
    gs[0:16, :] = jnp.exp(st_all[partner] - top) / total
    scale_peer = gs[...].T[0:n, :]
    gs[0:n, :] = scale_own
    gs[n:2 * n, :] = scale_peer
    lane = lax.broadcasted_iota(jnp.int32, (2 * n, LANES), 1)

    def y_copy(i, e):
        return rc(ysend.at[i, e], yrecv.at[i, e], s_y.at[i, e], r_y.at[i, e], y_peer)

    def scaled(i, yb, e):
        b = yb * 8 + c * 4 + i * 2 + e
        col = jnp.sum(jnp.where(lane == b, gs[...], 0.0), axis=1, keepdims=True)
        return col[0:n] * num_ref[b] + col[n:2 * n] * d2d[i, yb, e]

    def scale_step(i, carry):
        core_copy(i, 1 - y).wait_recv()
        for e in range(2):
            ysend[i, e] = scaled(i, 1 - y, e)
            y_copy(i, e).start()
        core_copy(i, y).wait_recv()
        for e in range(2):
            zsum[i, e] = scaled(i, y, e)
        return carry

    lax.fori_loop(0, 2, scale_step, 0)

    def y_add(i):
        for e in range(2):
            y_copy(i, e).wait_recv()
            zsum[i, e] = zsum[i, e] + yrecv[i, e]

    def chunk(ch):
        return pl.ds(pl.multiple_of(ch * rows, rows), rows)

    def z_end_send(i):
        def step(ch, carry):
            rc(zsum.at[i, e_far, chunk(ch)], rz_a.at[i, chunk(ch)], s_za.at[i, ch], r_za.at[i, ch], inward).start()
            return carry
        lax.fori_loop(0, NCH, step, 0)

    def z_mid(i):
        def near(ch, carry):
            cp = rc(rz_a.at[i, chunk(ch)], rz_b.at[i, chunk(ch)], s_za.at[i, ch], r_zb.at[i, ch], inward)
            rc(rz_a.at[i, chunk(ch)], rz_a.at[i, chunk(ch)], s_za.at[i, ch], r_za.at[i, ch], outward).wait_recv()
            rz_a[i, chunk(ch)] = rz_a[i, chunk(ch)] + zsum[i, e_far, chunk(ch)]
            cp.start()
            return carry

        def far(ch, carry):
            cp = rc(rz_b.at[i, chunk(ch)], rz_b.at[i, chunk(ch)], s_zb.at[i, ch], r_zb.at[i, ch], outward)
            cp.wait_recv()
            rz_b[i, chunk(ch)] = rz_b[i, chunk(ch)] + zsum[i, e_near, chunk(ch)]
            cp.start()
            return carry

        lax.fori_loop(0, NCH, near, 0)
        lax.fori_loop(0, NCH, far, 0)

    def z_end_recv(i):
        def step(ch, carry):
            rc(rz_b.at[i, chunk(ch)], rz_b.at[i, chunk(ch)], s_zb.at[i, ch], r_zb.at[i, ch], inward).wait_recv()
            return carry
        lax.fori_loop(0, NCH, step, 0)
        return rz_b[i] + zsum[i, e_near]

    def norm(index, values):
        return layer_norm(values, nlat_ref[index, 0:1, :], nlat_ref[index, 1:2, :])

    def attention(layer, xn):
        hd = wqkv.shape[2] // 6
        qkv = dot(xn, wqkv[layer]).astype(BF16)
        outs = []
        for h in range(2):
            q, k, v = (qkv[:, (2 * j + h) * hd:(2 * j + h + 1) * hd] for j in range(3))
            scores = dot_t(q, k) * (1.0 / math.sqrt(hd))
            weights = jnp.exp(scores - jnp.max(scores, axis=1, keepdims=True))
            probs = (weights / jnp.sum(weights, axis=1, keepdims=True)).astype(BF16)
            outs.append(dot(probs, v).astype(BF16))
        return dot(jnp.concatenate(outs, axis=1), lwo[layer])

    def mlp(layer, xn):
        return dot(gelu(dot(xn, lw1[layer])).astype(BF16), lw2[layer])

    kinds = (attention, mlp)

    def ln_near(u, ch):
        return ln_n.at[u, chunk(ch)]

    def source(kind, layer, u, s):
        values = zown[s]
        xn = norm(2 + 2 * layer + kind, values)
        ln_n[u] = xn.astype(F32)

        def send_ln(ch, carry):
            rc(ln_n.at[u, chunk(ch)], ln_n.at[u, chunk(ch)], s_lnn.at[u, ch], r_lnn.at[u, ch], inward).start()
            return carry

        lax.fori_loop(0, NCH, send_ln, 0)
        ac_n[u] = values + kinds[kind](layer, xn)

        def send_ac(ch, carry):
            rc(ac_n.at[u, chunk(ch)], ac_n.at[u, chunk(ch)], s_acn.at[u, ch], r_acn.at[u, ch], inward).start()
            return carry

        lax.fori_loop(0, NCH, send_ac, 0)

    def sink(kind, layer, u, s):
        def wait_ln(ch, carry):
            rc(ln_f.at[u, chunk(ch)], ln_f.at[u, chunk(ch)], s_lnf.at[u, ch], r_lnf.at[u, ch], inward).wait_recv()
            return carry

        lax.fori_loop(0, NCH, wait_ln, 0)
        part = kinds[kind](layer, ln_f[u].astype(BF16))

        def wait_ac(ch, carry):
            rc(ac_f.at[u, chunk(ch)], ac_f.at[u, chunk(ch)], s_acf.at[u, ch], r_acf.at[u, ch], inward).wait_recv()
            return carry

        lax.fori_loop(0, NCH, wait_ac, 0)
        zown[s] = ac_f[u] + part

    def middle(kind, layer, u):
        def near_ln(ch, carry):
            rc(ln_n.at[u, chunk(ch)], ln_n.at[u, chunk(ch)], s_lnn.at[u, ch], r_lnn.at[u, ch], outward).wait_recv()
            rc(ln_n.at[u, chunk(ch)], ln_f.at[u, chunk(ch)], s_lnn.at[u, ch], r_lnf.at[u, ch], inward).start()
            return carry

        lax.fori_loop(0, NCH, near_ln, 0)
        zown[0] = kinds[kind](layer, ln_n[u].astype(BF16))

        def both(ch, carry):
            cp = rc(ln_f.at[u, chunk(ch)], ln_f.at[u, chunk(ch)], s_lnf.at[u, ch], r_lnf.at[u, ch], outward)
            cp.wait_recv()
            cp.start()
            rc(ac_n.at[u, chunk(ch)], ac_n.at[u, chunk(ch)], s_acn.at[u, ch], r_acn.at[u, ch], outward).wait_recv()
            ac_n[u, chunk(ch)] = ac_n[u, chunk(ch)] + zown[0, chunk(ch)]
            rc(ac_n.at[u, chunk(ch)], ac_f.at[u, chunk(ch)], s_acn.at[u, ch], r_acf.at[u, ch], inward).start()
            return carry

        lax.fori_loop(0, NCH, both, 0)
        zown[1] = kinds[kind](layer, ln_f[u].astype(BF16))

        def far_ac(ch, carry):
            cp = rc(ac_f.at[u, chunk(ch)], ac_f.at[u, chunk(ch)], s_acf.at[u, ch], r_acf.at[u, ch], outward)
            cp.wait_recv()
            ac_f[u, chunk(ch)] = ac_f[u, chunk(ch)] + zown[1, chunk(ch)]
            cp.start()
            return carry

        lax.fori_loop(0, NCH, far_ac, 0)

    def line_seq(i, e):
        return y * 8 + c * 4 + i * 2 + e

    def ag_copy(b, ch, sems, dev):
        return rc(zall.at[b, chunk(ch)], zall.at[b, chunk(ch)], sems.at[b, ch], r_ag.at[b, ch], dev)

    def ag_send(b, ch, z_dev):
        if z_dev is not None:
            ag_copy(b, ch, s_agz, z_dev).start()
        ag_copy(b, ch, s_agy, y_peer).start()
        ag_copy(b, ch, s_agc, core_peer).start()

    def ag_source(i):
        b = line_seq(i, e_near)
        zall[b] = norm(6, zown[i]).astype(F32)

        def step(ch, carry):
            ag_send(b, ch, inward)
            return carry

        lax.fori_loop(0, NCH, step, 0)

    def ag_relay(i, e, z_dev):
        b = line_seq(i, e)

        def step(ch, carry):
            ag_copy(b, ch, s_agz, inward).wait_recv()
            ag_send(b, ch, z_dev)
            return carry

        lax.fori_loop(0, NCH, step, 0)

    def ag_cross(i, e):
        b = (1 - y) * 8 + c * 4 + i * 2 + e

        def step(ch, carry):
            ag_copy(b, ch, s_agy, y_peer).wait_recv()
            ag_copy(b, ch, s_agc, core_peer).start()
            return carry

        lax.fori_loop(0, NCH, step, 0)

    y_add(0)

    @pl.when(is_end)
    def _():
        z_end_send(0)

    @pl.when(is_mid)
    def _():
        z_mid(0)

    y_add(1)
    for load in loads:
        load.wait()

    @pl.when(is_end)
    def _():
        z_end_send(1)

        def start(s, carry):
            both = jnp.concatenate(split_bf16(z_end_recv(s)), axis=0)
            both = dot(both, wv[...])
            attended = (both[0:n] + both[n:2 * n]).astype(BF16)
            z = lat_ref[...].astype(F32) + dot(attended, wo[...])
            zown[s] = z + dot(gelu(dot(norm(1, z), emlp[0])).astype(BF16), emlp[1])
            source(0, 0, s, s)
            return carry

        lax.fori_loop(0, 2, start, 0)

        def layer_step(layer, carry):
            def attn_unit(s, inner):
                u = layer * 4 + s
                sink(0, layer, u, s)
                source(1, layer, u + 2, s)
                return inner

            lax.fori_loop(0, 2, attn_unit, 0)

            def mlp_unit(s, inner):
                u = layer * 4 + 2 + s
                sink(1, layer, u, s)

                @pl.when(layer == 0)
                def _():
                    source(0, 1, u + 2, s)

                @pl.when(layer == 1)
                def _():
                    ag_source(s)

                return inner

            lax.fori_loop(0, 2, mlp_unit, 0)
            return carry

        lax.fori_loop(0, 2, layer_step, 0)

    @pl.when(is_mid)
    def _():
        z_mid(1)

        def layer_step(layer, carry):
            for kind in range(2):
                def unit(s, inner):
                    middle(kind, layer, layer * 4 + 2 * kind + s)
                    return inner
                lax.fori_loop(0, 2, unit, 0)
            return carry

        lax.fori_loop(0, 2, layer_step, 0)

    def gather(i, carry):
        @pl.when(is_mid)
        def _():
            ag_relay(i, e_near, inward)
            ag_relay(i, e_far, outward)

        @pl.when(is_end)
        def _():
            ag_relay(i, e_far, None)

        ag_cross(i, e_near)
        ag_cross(i, e_far)
        return carry

    lax.fori_loop(0, 2, gather, 0)

    def last(k, carry):
        for yb in range(2):
            b = yb * 8 + (1 - c) * 4 + k

            def step(ch, inner):
                ag_copy(b, ch, s_agc, core_peer).wait_recv()
                return inner

            lax.fori_loop(0, NCH, step, 0)
        return carry

    lax.fori_loop(0, 4, last, 0)

    def convert(b, carry):
        out_ref[b] = zall[b].astype(BF16)
        return carry

    lax.fori_loop(0, 16, convert, 0)

    def done_stats(p, carry):
        g, dev = peer(p)
        rc(st_ref, st_all.at[me], s_st.at[g], r_st.at[me], dev).wait_send()
        return carry

    lax.fori_loop(1, 16, done_stats, 0)
    for i in range(2):
        core_copy(i, 1 - y).wait_send()
        core_copy(i, y).wait_send()
        for e in range(2):
            y_copy(i, e).wait_send()

    def done_z(i, carry):
        def step(ch, inner):
            rc(rz_a.at[i, chunk(ch)], rz_a.at[i, chunk(ch)], s_za.at[i, ch], r_za.at[i, ch], inward).wait_send()

            @pl.when(is_mid)
            def _():
                rc(rz_b.at[i, chunk(ch)], rz_b.at[i, chunk(ch)], s_zb.at[i, ch], r_zb.at[i, ch], outward).wait_send()

            return inner

        lax.fori_loop(0, NCH, step, 0)
        return carry

    lax.fori_loop(0, 2, done_z, 0)

    def done_units(u, carry):
        def step(ch, inner):
            rc(ln_n.at[u, chunk(ch)], ln_n.at[u, chunk(ch)], s_lnn.at[u, ch], r_lnn.at[u, ch], inward).wait_send()
            rc(ac_n.at[u, chunk(ch)], ac_n.at[u, chunk(ch)], s_acn.at[u, ch], r_acn.at[u, ch], inward).wait_send()

            @pl.when(is_mid)
            def _():
                rc(ln_f.at[u, chunk(ch)], ln_f.at[u, chunk(ch)], s_lnf.at[u, ch], r_lnf.at[u, ch], outward).wait_send()
                rc(ac_f.at[u, chunk(ch)], ac_f.at[u, chunk(ch)], s_acf.at[u, ch], r_acf.at[u, ch], outward).wait_send()

            return inner

        lax.fori_loop(0, NCH, step, 0)
        return carry

    lax.fori_loop(0, 8, done_units, 0)

    def done_ag(i, carry):
        for e in range(2):
            b = line_seq(i, e)
            other = (1 - y) * 8 + c * 4 + i * 2 + e

            def step(ch, inner):
                ag_copy(b, ch, s_agy, y_peer).wait_send()
                ag_copy(b, ch, s_agc, core_peer).wait_send()
                ag_copy(other, ch, s_agc, core_peer).wait_send()

                @pl.when(jnp.logical_or(is_mid, e == e_near))
                def _():
                    ag_copy(b, ch, s_agz, inward).wait_send()

                return inner

            lax.fori_loop(0, NCH, step, 0)
        return carry

    lax.fori_loop(0, 2, done_ag, 0)


def latent_all(num, stats, latents, norm_lat, enc_wkv, enc_wo, enc_mlp, wqkv, lwo, lw1, lw2):
    nb, n, dim = num.shape
    vm = pl.BlockSpec(memory_space=pltpu.VMEM)
    hbm = pl.BlockSpec(memory_space=pl.ANY)
    dma = pltpu.SemaphoreType.DMA
    buf = lambda *shape: pltpu.VMEM(shape + (n, dim), F32)
    return pl.pallas_call(
        latent_kernel,
        in_specs=[vm] * 4 + [hbm] * 7,
        out_specs=vm,
        out_shape=jax.ShapeDtypeStruct((nb, n, dim), BF16),
        scratch_shapes=[
            pltpu.VMEM((dim, dim), BF16), pltpu.VMEM((dim, dim), BF16), pltpu.VMEM(enc_mlp.shape, BF16),
            pltpu.VMEM(wqkv.shape, BF16), pltpu.VMEM(lwo.shape, BF16), pltpu.VMEM(lw1.shape, BF16), pltpu.VMEM(lw2.shape, BF16),
            dma((7,)),
            pltpu.VMEM((16, nb, LANES), F32), pltpu.VMEM((LANES, LANES), F32),
            buf(2, 2, 2), buf(2, 2), buf(2, 2), buf(2, 2), buf(2), buf(2),
            buf(8), buf(8), buf(8), buf(8), buf(2), buf(nb),
            dma((16,)), dma((16,)), dma((2, 2)), dma((2, 2)), dma((2, 2)), dma((2, 2)),
            dma((2, NCH)), dma((2, NCH)), dma((2, NCH)), dma((2, NCH)),
        ] + [dma((8, NCH))] * 8 + [dma((nb, NCH))] * 4,
        compiler_params=pltpu.CompilerParams(vmem_limit_bytes=VMEM_LIMIT, collective_id=0, has_side_effects=True),
        name='latent_all',
    )(num, stats, latents, norm_lat, enc_wkv, enc_wo, enc_mlp, wqkv, lwo, lw1, lw2)


def decoder_kernel(q_ref, zn_ref, nq_ref, nm_ref, wq_ref, wkv_ref, wo_ref, mlp_ref, wout_ref, y_ref, kq_s, vo_s):
    b = pl.program_id(0)
    nb, n, dim = zn_ref.shape

    @pl.when(b == 0)
    def _():
        def prepare(k, carry):
            zn = zn_ref[pl.ds(k * 4, 4)].reshape(4 * n, dim)
            high, low = split_bf16(dot_t(dot(zn, wkv_ref[0]).astype(BF16), wq_ref[...]))
            kq_s[pl.ds(k * 4, 4), 0:n, :] = high.reshape(4, n, dim)
            kq_s[pl.ds(k * 4, 4), n:2 * n, :] = low.reshape(4, n, dim)
            high, low = split_bf16(dot(dot(zn, wkv_ref[1]).astype(BF16), wo_ref[...]))
            vo_s[pl.ds(k * 4, 4), 0:n, :] = high.reshape(4, n, dim)
            vo_s[pl.ds(k * 4, 4), n:2 * n, :] = low.reshape(4, n, dim)
            return carry

        lax.fori_loop(0, nb // 4, prepare, 0)

    xq = layer_norm(q_ref[0].astype(F32), nq_ref[0:1, :], nq_ref[1:2, :])
    both = dot_t(xq, kq_s[b])
    scores = (both + pltpu.roll(both, n, 1)) * (1.0 / math.sqrt(dim))
    weights = jnp.exp(scores - jnp.max(scores, axis=1, keepdims=True))
    probs = (weights / (0.5 * jnp.sum(weights, axis=1, keepdims=True))).astype(BF16)
    u = dot(probs, vo_s[b])
    hidden = gelu(dot(layer_norm(u, nm_ref[0:1, :], nm_ref[1:2, :]), mlp_ref[0])).astype(BF16)
    u = u + dot(hidden, mlp_ref[1])
    y_ref[0] = dot(u.astype(BF16), wout_ref[...])


def decoder(q_loc, zn, norm_query, norm_mlp, dec_wq, dec_wkv, dec_wo, dec_mlp, dec_out):
    nb, rows, dim = q_loc.shape
    n = zn.shape[1]
    whole = lambda shape: pl.BlockSpec(shape, lambda b: (0,) * len(shape), pipeline_mode=pl.Buffered(1))
    return pl.pallas_call(
        decoder_kernel,
        grid=(nb,),
        in_specs=[pl.BlockSpec((1, rows, dim), lambda b: (b, 0, 0)), whole(zn.shape), whole((2, dim)), whole((2, dim)),
                  whole((dim, dim)), whole((2, dim, dim)), whole((dim, dim)), whole((2, dim, dim)), whole((dim, dim))],
        out_specs=pl.BlockSpec((1, rows, dim), lambda b: (b, 0, 0)),
        out_shape=jax.ShapeDtypeStruct((nb, rows, dim), F32),
        scratch_shapes=[pltpu.VMEM((nb, 2 * n, dim), BF16), pltpu.VMEM((nb, 2 * n, dim), BF16)],
        compiler_params=pltpu.CompilerParams(vmem_limit_bytes=VMEM_LIMIT),
        name='dec_local',
    )(q_loc, zn, norm_query, norm_mlp, dec_wq, dec_wkv, dec_wo, dec_mlp, dec_out)


def solution(mesh):
    seq_spec = P('dp', ('tp', 'sp'), None)
    replicated = P()
    in_specs = (seq_spec, seq_spec, replicated, replicated, replicated, replicated, replicated, replicated, replicated, replicated,
                P(None, None, None, 'tp', None), P(None, 'tp', None, None), P(None, None, 'tp'), P(None, 'tp', None),
                replicated, replicated, replicated, replicated, replicated)

    def device_step(x_loc, q_loc, latents, norm_in, norm_query, norm_lat, enc_wq, enc_wkv, enc_wo, enc_mlp,
                    lat_wqkv, lat_wo, lat_w1, lat_w2, dec_wq, dec_wkv, dec_wo, dec_mlp, dec_out):
        layers, dim = lat_wqkv.shape[0], latents.shape[1]
        wqkv = lat_wqkv.reshape(layers, dim, -1)
        lwo = lat_wo.reshape(layers, -1, dim)
        num, stats = encoder_local(x_loc, norm_in, latents, norm_lat[0], enc_wq, enc_wkv)
        zn = latent_all(num, stats, latents, norm_lat, enc_wkv, enc_wo, enc_mlp, wqkv, lwo, lat_w1, lat_w2)
        return decoder(q_loc, zn, norm_query, norm_lat[7], dec_wq, dec_wkv, dec_wo, dec_mlp, dec_out)

    return jax.shard_map(device_step, mesh=mesh, in_specs=in_specs, out_specs=seq_spec, check_vma=False)
```

```python
import functools
import math
import jax
import jax.numpy as jnp
from jax import lax
from jax.experimental import pallas as pl
from jax.experimental.pallas import tpu as pltpu
from jax.sharding import PartitionSpec as P

LN_EPS = 1e-5
F32, BF16 = jnp.float32, jnp.bfloat16
MESH = pl.DeviceIdType.MESH
VMEM_LIMIT = 60 * 1024 * 1024
LANES = 128
NLINE = 4
RBLK = 128
ENC_STEP = 4
NCH = 4
GELU_C = math.sqrt(2.0 / math.pi)


def layer_norm(values, gain, bias):
    row_mean = jnp.mean(values, axis=-1, keepdims=True)
    centered = values - row_mean
    row_var = jnp.mean(centered * centered, axis=-1, keepdims=True)
    return (centered * lax.rsqrt(row_var + LN_EPS) * gain + bias).astype(BF16)


def gelu(x):
    return 0.5 * x * (1.0 + jnp.tanh(GELU_C * (x + 0.044715 * (x * x * x))))


def dot(a, b):
    return jnp.dot(a, b, preferred_element_type=F32)


def dot_t(a, b):
    return lax.dot_general(a, b, (((1,), (1,)), ((), ())), preferred_element_type=F32)


def split_bf16(x):
    high = x.astype(BF16)
    return high, (x - high.astype(F32)).astype(BF16)


def encoder_kernel(x_ref, nin_ref, lat_ref, nq_ref, wq_ref, wk_ref, num_ref, st_ref, qk_s, stats_s):
    b = pl.program_id(0)
    n = lat_ref.shape[0]
    dim = lat_ref.shape[1]

    @pl.when(b == 0)
    def _():
        q = dot(layer_norm(lat_ref[...].astype(F32), nq_ref[0:1, :], nq_ref[1:2, :]), wq_ref[...]).astype(BF16)
        high, low = split_bf16(dot_t(q, wk_ref[0]))
        qk_s[0:n, :] = high
        qk_s[n:2 * n, :] = low
        stats_s[...] = jnp.zeros_like(stats_s)

    each = range(x_ref.shape[0])
    xns = [layer_norm(x_ref[j].astype(F32), nin_ref[0:1, :], nin_ref[1:2, :]) for j in each]
    both = [dot_t(qk_s[...], xn) for xn in xns]
    scores = [(v[:n] + v[n:]) * (1.0 / math.sqrt(dim)) for v in both]
    maxima = [jnp.max(v, axis=1, keepdims=True) for v in scores]
    weights = [jnp.exp(v - m) for v, m in zip(scores, maxima)]
    sums = [jnp.sum(v, axis=1, keepdims=True) for v in weights]
    for j in each:
        num_ref[j] = dot(weights[j].astype(BF16), xns[j])
        here = lax.broadcasted_iota(jnp.int32, (n, LANES), 1) == b * x_ref.shape[0] + j
        stats_s[0:n, :] = jnp.where(here, maxima[j], stats_s[0:n, :])
        stats_s[n:2 * n, :] = jnp.where(here, sums[j], stats_s[n:2 * n, :])

    @pl.when(b == pl.num_programs(0) - 1)
    def _():
        st_ref[...] = stats_s[...].T[0:st_ref.shape[0], :]


def encoder_local(x_loc, norm_in, latents, norm_q, enc_wq, enc_wkv):
    nb, rows, dim = x_loc.shape
    n = latents.shape[0]
    whole = lambda shape: pl.BlockSpec(shape, lambda b: (0,) * len(shape))
    return pl.pallas_call(
        encoder_kernel,
        grid=(nb // ENC_STEP,),
        in_specs=[pl.BlockSpec((ENC_STEP, rows, dim), lambda b: (b, 0, 0)), whole((2, dim)), whole((n, dim)), whole((2, dim)),
                  whole((dim, dim)), pl.BlockSpec((1, dim, dim), lambda b: (0, 0, 0))],
        out_specs=[pl.BlockSpec((ENC_STEP, n, dim), lambda b: (b, 0, 0)), whole((nb, LANES))],
        out_shape=[jax.ShapeDtypeStruct((nb, n, dim), F32), jax.ShapeDtypeStruct((nb, LANES), F32)],
        scratch_shapes=[pltpu.VMEM((2 * n, dim), BF16), pltpu.VMEM((LANES, LANES), F32)],
        compiler_params=pltpu.CompilerParams(vmem_limit_bytes=VMEM_LIMIT),
        name='enc_local',
    )(x_loc, norm_in, latents, norm_q, enc_wq, enc_wkv)


def latent_kernel(num_ref, st_ref, lat_ref, nlat_ref, wkv_h, wo_h, emlp_h, qkv_h, lwo_h, lw1_h, lw2_h, out_ref,
                  wv, wo, emlp, wqkv, lwo, lw1, lw2, wsem,
                  st_all, gs, d2d, ysend, yrecv, zsum, rz_a, rz_b, ln_n, ln_f, ac_n, ac_f, zown, zall,
                  s_st, r_st, s_d2, r_d2, s_y, r_y, s_za, s_zb, r_za, r_zb,
                  s_lnn, s_lnf, s_acn, s_acf, r_lnn, r_lnf, r_acn, r_acf, r_ag, s_agz, s_agc, s_agy):
    n, dim = lat_ref.shape
    rows = n // NCH
    x = lax.axis_index('dp')
    t = lax.axis_index('tp')
    sp = lax.axis_index('sp')
    y = lax.div(sp, 2)
    c = lax.rem(sp, 2)
    me = t * 4 + sp
    upper = lax.div(t, 2)
    is_end = jnp.logical_or(t == 0, t == NLINE - 1)
    is_mid = jnp.logical_not(is_end)
    e_near = upper
    e_far = 1 - upper
    inward = (x, jnp.where(t == 0, 1, jnp.where(t == 1, 2, jnp.where(t == 2, 1, 2))), sp)
    outward = (x, jnp.where(t <= 1, 0, NLINE - 1), sp)
    core_peer = (x, t, y * 2 + (1 - c))
    y_peer = (x, t, (1 - y) * 2 + c)

    def rc(src, dst, ssem, rsem, dev):
        return pltpu.make_async_remote_copy(src_ref=src, dst_ref=dst, send_sem=ssem, recv_sem=rsem,
                                            device_id=dev, device_id_type=MESH)

    def peer(p):
        g = lax.rem(me + p, 16)
        return g, (x, lax.div(g, 4), lax.rem(g, 4))

    loads = [pltpu.make_async_copy(src, dst, wsem.at[i]) for i, (src, dst) in enumerate(
        ((wkv_h.at[1], wv), (wo_h, wo), (emlp_h, emlp), (qkv_h, wqkv), (lwo_h, lwo), (lw1_h, lw1), (lw2_h, lw2)))]
    for load in loads:
        load.start()

    barrier = pltpu.get_barrier_semaphore()

    def greet(p, carry):
        pl.semaphore_signal(barrier, inc=1, device_id=peer(p)[1], device_id_type=MESH)
        return carry

    lax.fori_loop(1, 16, greet, 0)
    pl.semaphore_wait(barrier, 15)

    def send_stats(p, carry):
        g, dev = peer(p)
        rc(st_ref, st_all.at[me], s_st.at[g], r_st.at[me], dev).start()
        return carry

    lax.fori_loop(1, 16, send_stats, 0)

    def core_copy(i, yb):
        return rc(num_ref.at[pl.ds(yb * 8 + (1 - c) * 4 + i * 2, 2)], d2d.at[i, yb], s_d2.at[i, yb], r_d2.at[i, yb], core_peer)

    for i in range(2):
        core_copy(i, 1 - y).start()
        core_copy(i, y).start()
    st_all[me] = st_ref[...]

    def wait_stats(p, carry):
        g, dev = peer(p)
        rc(st_ref, st_all.at[g], s_st.at[g], r_st.at[g], dev).wait_recv()
        return carry

    lax.fori_loop(1, 16, wait_stats, 0)
    top = lax.fori_loop(1, 16, lambda d, m: jnp.maximum(m, st_all[d]), st_all[0])

    def add_sum(d, total):
        stats = st_all[d]
        return total + jnp.exp(stats - top) * pltpu.roll(stats, n, 1)

    total = lax.fori_loop(0, 16, add_sum, jnp.zeros_like(top))
    partner = t * 4 + y * 2 + (1 - c)
    gs[...] = jnp.zeros_like(gs)
    gs[0:16, :] = jnp.exp(st_all[me] - top) / total
    scale_own = gs[...].T[0:n, :]
    gs[0:16, :] = jnp.exp(st_all[partner] - top) / total
    scale_peer = gs[...].T[0:n, :]
    gs[0:n, :] = scale_own
    gs[n:2 * n, :] = scale_peer
    lane = lax.broadcasted_iota(jnp.int32, (2 * n, LANES), 1)

    def y_copy(i, e):
        return rc(ysend.at[i, e], yrecv.at[i, e], s_y.at[i, e], r_y.at[i, e], y_peer)

    def scaled(i, yb, e):
        b = yb * 8 + c * 4 + i * 2 + e
        col = jnp.sum(jnp.where(lane == b, gs[...], 0.0), axis=1, keepdims=True)
        return col[0:n] * num_ref[b] + col[n:2 * n] * d2d[i, yb, e]

    def scale_step(i, carry):
        core_copy(i, 1 - y).wait_recv()
        for e in range(2):
            ysend[i, e] = scaled(i, 1 - y, e)
            y_copy(i, e).start()
        core_copy(i, y).wait_recv()
        for e in range(2):
            zsum[i, e] = scaled(i, y, e)
        return carry

    lax.fori_loop(0, 2, scale_step, 0)

    def y_add(i):
        for e in range(2):
            y_copy(i, e).wait_recv()
            zsum[i, e] = zsum[i, e] + yrecv[i, e]

    def chunk(ch):
        return pl.ds(pl.multiple_of(ch * rows, rows), rows)

    def z_end_send(i):
        def step(ch, carry):
            rc(zsum.at[i, e_far, chunk(ch)], rz_a.at[i, chunk(ch)], s_za.at[i, ch], r_za.at[i, ch], inward).start()
            return carry
        lax.fori_loop(0, NCH, step, 0)

    def z_mid(i):
        def near(ch, carry):
            cp = rc(rz_a.at[i, chunk(ch)], rz_b.at[i, chunk(ch)], s_za.at[i, ch], r_zb.at[i, ch], inward)
            rc(rz_a.at[i, chunk(ch)], rz_a.at[i, chunk(ch)], s_za.at[i, ch], r_za.at[i, ch], outward).wait_recv()
            rz_a[i, chunk(ch)] = rz_a[i, chunk(ch)] + zsum[i, e_far, chunk(ch)]
            cp.start()
            return carry

        def far(ch, carry):
            cp = rc(rz_b.at[i, chunk(ch)], rz_b.at[i, chunk(ch)], s_zb.at[i, ch], r_zb.at[i, ch], outward)
            cp.wait_recv()
            rz_b[i, chunk(ch)] = rz_b[i, chunk(ch)] + zsum[i, e_near, chunk(ch)]
            cp.start()
            return carry

        lax.fori_loop(0, NCH, near, 0)
        lax.fori_loop(0, NCH, far, 0)

    def z_end_recv(i):
        def step(ch, carry):
            rc(rz_b.at[i, chunk(ch)], rz_b.at[i, chunk(ch)], s_zb.at[i, ch], r_zb.at[i, ch], inward).wait_recv()
            return carry
        lax.fori_loop(0, NCH, step, 0)
        return rz_b[i] + zsum[i, e_near]

    def norm(index, values):
        return layer_norm(values, nlat_ref[index, 0:1, :], nlat_ref[index, 1:2, :])

    def attention(layer, xn):
        hd = wqkv.shape[4]
        qkv = [dot(xn, jnp.concatenate([wqkv[layer, j, 0], wqkv[layer, j, 1]], axis=1)).astype(BF16) for j in range(3)]
        outs = []
        for h in range(2):
            q, k, v = (part[:, h * hd:(h + 1) * hd] for part in qkv)
            scores = dot_t(q, k) * (1.0 / math.sqrt(hd))
            weights = jnp.exp(scores - jnp.max(scores, axis=1, keepdims=True))
            probs = (weights / jnp.sum(weights, axis=1, keepdims=True)).astype(BF16)
            outs.append(dot(probs, v).astype(BF16))
        return dot(jnp.concatenate(outs, axis=1), lwo[layer])

    def mlp(layer, xn):
        return dot(gelu(dot(xn, lw1[layer])).astype(BF16), lw2[layer])

    kinds = (attention, mlp)

    def ln_near(u, ch):
        return ln_n.at[u, chunk(ch)]

    def source(kind, layer, u, s):
        values = zown[s]
        xn = norm(2 + 2 * layer + kind, values)
        ln_n[u] = xn.astype(F32)

        def send_ln(ch, carry):
            rc(ln_n.at[u, chunk(ch)], ln_n.at[u, chunk(ch)], s_lnn.at[u, ch], r_lnn.at[u, ch], inward).start()
            return carry

        lax.fori_loop(0, NCH, send_ln, 0)
        ac_n[u] = values + kinds[kind](layer, xn)

        def send_ac(ch, carry):
            rc(ac_n.at[u, chunk(ch)], ac_n.at[u, chunk(ch)], s_acn.at[u, ch], r_acn.at[u, ch], inward).start()
            return carry

        lax.fori_loop(0, NCH, send_ac, 0)

    def sink(kind, layer, u, s):
        def wait_ln(ch, carry):
            rc(ln_f.at[u, chunk(ch)], ln_f.at[u, chunk(ch)], s_lnf.at[u, ch], r_lnf.at[u, ch], inward).wait_recv()
            return carry

        lax.fori_loop(0, NCH, wait_ln, 0)
        part = kinds[kind](layer, ln_f[u].astype(BF16))

        def wait_ac(ch, carry):
            rc(ac_f.at[u, chunk(ch)], ac_f.at[u, chunk(ch)], s_acf.at[u, ch], r_acf.at[u, ch], inward).wait_recv()
            return carry

        lax.fori_loop(0, NCH, wait_ac, 0)
        zown[s] = ac_f[u] + part

    def middle(kind, layer, u):
        def near_ln(ch, carry):
            rc(ln_n.at[u, chunk(ch)], ln_n.at[u, chunk(ch)], s_lnn.at[u, ch], r_lnn.at[u, ch], outward).wait_recv()
            rc(ln_n.at[u, chunk(ch)], ln_f.at[u, chunk(ch)], s_lnn.at[u, ch], r_lnf.at[u, ch], inward).start()
            return carry

        lax.fori_loop(0, NCH, near_ln, 0)
        zown[0] = kinds[kind](layer, ln_n[u].astype(BF16))

        def both(ch, carry):
            cp = rc(ln_f.at[u, chunk(ch)], ln_f.at[u, chunk(ch)], s_lnf.at[u, ch], r_lnf.at[u, ch], outward)
            cp.wait_recv()
            cp.start()
            rc(ac_n.at[u, chunk(ch)], ac_n.at[u, chunk(ch)], s_acn.at[u, ch], r_acn.at[u, ch], outward).wait_recv()
            ac_n[u, chunk(ch)] = ac_n[u, chunk(ch)] + zown[0, chunk(ch)]
            rc(ac_n.at[u, chunk(ch)], ac_f.at[u, chunk(ch)], s_acn.at[u, ch], r_acf.at[u, ch], inward).start()
            return carry

        lax.fori_loop(0, NCH, both, 0)
        zown[1] = kinds[kind](layer, ln_f[u].astype(BF16))

        def far_ac(ch, carry):
            cp = rc(ac_f.at[u, chunk(ch)], ac_f.at[u, chunk(ch)], s_acf.at[u, ch], r_acf.at[u, ch], outward)
            cp.wait_recv()
            ac_f[u, chunk(ch)] = ac_f[u, chunk(ch)] + zown[1, chunk(ch)]
            cp.start()
            return carry

        lax.fori_loop(0, NCH, far_ac, 0)

    def line_seq(i, e):
        return y * 8 + c * 4 + i * 2 + e

    def ag_copy(b, ch, sems, dev):
        return rc(zall.at[b, chunk(ch)], zall.at[b, chunk(ch)], sems.at[b, ch], r_ag.at[b, ch], dev)

    def ag_send(b, ch, z_dev):
        if z_dev is not None:
            ag_copy(b, ch, s_agz, z_dev).start()
        ag_copy(b, ch, s_agy, y_peer).start()
        ag_copy(b, ch, s_agc, core_peer).start()

    def ag_source(i):
        b = line_seq(i, e_near)
        zall[b] = norm(6, zown[i]).astype(F32)

        def step(ch, carry):
            ag_send(b, ch, inward)
            return carry

        lax.fori_loop(0, NCH, step, 0)

    def ag_relay(i, e, z_dev):
        b = line_seq(i, e)

        def step(ch, carry):
            ag_copy(b, ch, s_agz, inward).wait_recv()
            ag_send(b, ch, z_dev)
            return carry

        lax.fori_loop(0, NCH, step, 0)

    def ag_cross(i, e):
        b = (1 - y) * 8 + c * 4 + i * 2 + e

        def step(ch, carry):
            ag_copy(b, ch, s_agy, y_peer).wait_recv()
            ag_copy(b, ch, s_agc, core_peer).start()
            return carry

        lax.fori_loop(0, NCH, step, 0)

    y_add(0)

    @pl.when(is_end)
    def _():
        z_end_send(0)

    @pl.when(is_mid)
    def _():
        z_mid(0)

    y_add(1)
    for load in loads:
        load.wait()

    @pl.when(is_end)
    def _():
        z_end_send(1)

        def start(s, carry):
            both = jnp.concatenate(split_bf16(z_end_recv(s)), axis=0)
            both = dot(both, wv[...])
            attended = (both[0:n] + both[n:2 * n]).astype(BF16)
            z = lat_ref[...].astype(F32) + dot(attended, wo[...])
            zown[s] = z + dot(gelu(dot(norm(1, z), emlp[0])).astype(BF16), emlp[1])
            source(0, 0, s, s)
            return carry

        lax.fori_loop(0, 2, start, 0)

        def layer_step(layer, carry):
            def attn_unit(s, inner):
                u = layer * 4 + s
                sink(0, layer, u, s)
                source(1, layer, u + 2, s)
                return inner

            lax.fori_loop(0, 2, attn_unit, 0)

            def mlp_unit(s, inner):
                u = layer * 4 + 2 + s
                sink(1, layer, u, s)

                @pl.when(layer == 0)
                def _():
                    source(0, 1, u + 2, s)

                @pl.when(layer == 1)
                def _():
                    ag_source(s)

                return inner

            lax.fori_loop(0, 2, mlp_unit, 0)
            return carry

        lax.fori_loop(0, 2, layer_step, 0)

    @pl.when(is_mid)
    def _():
        z_mid(1)

        def layer_step(layer, carry):
            for kind in range(2):
                def unit(s, inner):
                    middle(kind, layer, layer * 4 + 2 * kind + s)
                    return inner
                lax.fori_loop(0, 2, unit, 0)
            return carry

        lax.fori_loop(0, 2, layer_step, 0)

    def gather(i, carry):
        @pl.when(is_mid)
        def _():
            ag_relay(i, e_near, inward)
            ag_relay(i, e_far, outward)

        @pl.when(is_end)
        def _():
            ag_relay(i, e_far, None)

        ag_cross(i, e_near)
        ag_cross(i, e_far)
        return carry

    lax.fori_loop(0, 2, gather, 0)

    def last(k, carry):
        for yb in range(2):
            b = yb * 8 + (1 - c) * 4 + k

            def step(ch, inner):
                ag_copy(b, ch, s_agc, core_peer).wait_recv()
                return inner

            lax.fori_loop(0, NCH, step, 0)
        return carry

    lax.fori_loop(0, 4, last, 0)

    def convert(b, carry):
        out_ref[b] = zall[b].astype(BF16)
        return carry

    lax.fori_loop(0, 16, convert, 0)

    def done_stats(p, carry):
        g, dev = peer(p)
        rc(st_ref, st_all.at[me], s_st.at[g], r_st.at[me], dev).wait_send()
        return carry

    lax.fori_loop(1, 16, done_stats, 0)
    for i in range(2):
        core_copy(i, 1 - y).wait_send()
        core_copy(i, y).wait_send()
        for e in range(2):
            y_copy(i, e).wait_send()

    def done_z(i, carry):
        def step(ch, inner):
            rc(rz_a.at[i, chunk(ch)], rz_a.at[i, chunk(ch)], s_za.at[i, ch], r_za.at[i, ch], inward).wait_send()

            @pl.when(is_mid)
            def _():
                rc(rz_b.at[i, chunk(ch)], rz_b.at[i, chunk(ch)], s_zb.at[i, ch], r_zb.at[i, ch], outward).wait_send()

            return inner

        lax.fori_loop(0, NCH, step, 0)
        return carry

    lax.fori_loop(0, 2, done_z, 0)

    def done_units(u, carry):
        def step(ch, inner):
            rc(ln_n.at[u, chunk(ch)], ln_n.at[u, chunk(ch)], s_lnn.at[u, ch], r_lnn.at[u, ch], inward).wait_send()
            rc(ac_n.at[u, chunk(ch)], ac_n.at[u, chunk(ch)], s_acn.at[u, ch], r_acn.at[u, ch], inward).wait_send()

            @pl.when(is_mid)
            def _():
                rc(ln_f.at[u, chunk(ch)], ln_f.at[u, chunk(ch)], s_lnf.at[u, ch], r_lnf.at[u, ch], outward).wait_send()
                rc(ac_f.at[u, chunk(ch)], ac_f.at[u, chunk(ch)], s_acf.at[u, ch], r_acf.at[u, ch], outward).wait_send()

            return inner

        lax.fori_loop(0, NCH, step, 0)
        return carry

    lax.fori_loop(0, 8, done_units, 0)

    def done_ag(i, carry):
        for e in range(2):
            b = line_seq(i, e)
            other = (1 - y) * 8 + c * 4 + i * 2 + e

            def step(ch, inner):
                ag_copy(b, ch, s_agy, y_peer).wait_send()
                ag_copy(b, ch, s_agc, core_peer).wait_send()
                ag_copy(other, ch, s_agc, core_peer).wait_send()

                @pl.when(jnp.logical_or(is_mid, e == e_near))
                def _():
                    ag_copy(b, ch, s_agz, inward).wait_send()

                return inner

            lax.fori_loop(0, NCH, step, 0)
        return carry

    lax.fori_loop(0, 2, done_ag, 0)


def latent_all(num, stats, latents, norm_lat, enc_wkv, enc_wo, enc_mlp, wqkv, lwo, lw1, lw2):
    nb, n, dim = num.shape
    vm = pl.BlockSpec(memory_space=pltpu.VMEM)
    hbm = pl.BlockSpec(memory_space=pl.ANY)
    dma = pltpu.SemaphoreType.DMA
    buf = lambda *shape: pltpu.VMEM(shape + (n, dim), F32)
    return pl.pallas_call(
        latent_kernel,
        in_specs=[vm] * 4 + [hbm] * 7,
        out_specs=vm,
        out_shape=jax.ShapeDtypeStruct((nb, n, dim), BF16),
        scratch_shapes=[
            pltpu.VMEM((dim, dim), BF16), pltpu.VMEM((dim, dim), BF16), pltpu.VMEM(enc_mlp.shape, BF16),
            pltpu.VMEM(wqkv.shape, BF16), pltpu.VMEM(lwo.shape, BF16), pltpu.VMEM(lw1.shape, BF16), pltpu.VMEM(lw2.shape, BF16),
            dma((7,)),
            pltpu.VMEM((16, nb, LANES), F32), pltpu.VMEM((LANES, LANES), F32),
            buf(2, 2, 2), buf(2, 2), buf(2, 2), buf(2, 2), buf(2), buf(2),
            buf(8), buf(8), buf(8), buf(8), buf(2), buf(nb),
            dma((16,)), dma((16,)), dma((2, 2)), dma((2, 2)), dma((2, 2)), dma((2, 2)),
            dma((2, NCH)), dma((2, NCH)), dma((2, NCH)), dma((2, NCH)),
        ] + [dma((8, NCH))] * 8 + [dma((nb, NCH))] * 4,
        compiler_params=pltpu.CompilerParams(vmem_limit_bytes=VMEM_LIMIT, collective_id=0, has_side_effects=True),
        name='latent_all',
    )(num, stats, latents, norm_lat, enc_wkv, enc_wo, enc_mlp, wqkv, lwo, lw1, lw2)


def decoder_kernel(q_ref, zn_ref, nq_ref, nm_ref, wq_ref, wkv_ref, wo_ref, mlp_ref, wout_ref, y_ref, kq_s, vo_s, xu_s, u_s, p_s):
    b = pl.program_id(0)
    nb, n, dim = zn_ref.shape

    @pl.when(b == 0)
    def _():
        def prepare(k, carry):
            zn = zn_ref[pl.ds(k * 4, 4)].reshape(4 * n, dim)
            high, low = split_bf16(dot_t(dot(zn, wkv_ref[0]).astype(BF16), wq_ref[...]))
            kq_s[pl.ds(k * 4, 4), 0:n, :] = high.reshape(4, n, dim)
            kq_s[pl.ds(k * 4, 4), n:2 * n, :] = low.reshape(4, n, dim)
            high, low = split_bf16(dot(dot(zn, wkv_ref[1]).astype(BF16), wo_ref[...]))
            vo_s[pl.ds(k * 4, 4), 0:n, :] = high.reshape(4, n, dim)
            vo_s[pl.ds(k * 4, 4), n:2 * n, :] = low.reshape(4, n, dim)
            return carry

        lax.fori_loop(0, nb // 4, prepare, 0)
        xu_s[...] = jnp.zeros_like(xu_s)
        u_s[...] = jnp.zeros_like(u_s)

    ahead = lax.rem(b, 2)
    now = 1 - ahead
    seq = jnp.minimum(b, nb - 1)
    rows = q_ref.shape[1]
    nblk = rows // RBLK
    cblk = dim // nblk
    xu = xu_s[now]
    hidden = []
    for k in range(nblk):
        part = pl.ds(k * RBLK, RBLK)
        cols = slice(k * cblk, (k + 1) * cblk)
        hidden.append(gelu(dot(xu, mlp_ref[0, :, cols])).astype(BF16))
        xq = layer_norm(q_ref[0, part].astype(F32), nq_ref[0:1, :], nq_ref[1:2, :])
        both = dot_t(xq, kq_s[seq])
        scores = (both + pltpu.roll(both, n, 1)) * (1.0 / math.sqrt(dim))
        weights = jnp.exp(scores - jnp.max(scores, axis=1, keepdims=True))
        probs = (weights / (0.5 * jnp.sum(weights, axis=1, keepdims=True))).astype(BF16)
        p_s[part] = probs
    hidden = jnp.concatenate(hidden, axis=1)
    out = []
    for k in range(nblk):
        part = pl.ds(k * RBLK, RBLK)
        cols = slice(k * cblk, (k + 1) * cblk)
        out.append((u_s[now, :, cols] + dot(hidden, mlp_ref[1, :, cols])).astype(BF16))
        u = dot(p_s[part], vo_s[seq])
        u_s[ahead, part] = u
        xu_s[ahead, part] = layer_norm(u, nm_ref[0:1, :], nm_ref[1:2, :])
    out = jnp.concatenate(out, axis=1)
    y_ref[0] = dot(out, wout_ref[...])


def decoder(q_loc, zn, norm_query, norm_mlp, dec_wq, dec_wkv, dec_wo, dec_mlp, dec_out):
    nb, rows, dim = q_loc.shape
    n = zn.shape[1]
    whole = lambda shape: pl.BlockSpec(shape, lambda b: (0,) * len(shape), pipeline_mode=pl.Buffered(1))
    return pl.pallas_call(
        decoder_kernel,
        grid=(nb + 1,),
        in_specs=[pl.BlockSpec((1, rows, dim), lambda b: (jnp.minimum(b, nb - 1), 0, 0)), whole(zn.shape), whole((2, dim)), whole((2, dim)),
                  whole((dim, dim)), whole((2, dim, dim)), whole((dim, dim)), whole((2, dim, dim)), whole((dim, dim))],
        out_specs=pl.BlockSpec((1, rows, dim), lambda b: (jnp.maximum(b - 1, 0), 0, 0)),
        out_shape=jax.ShapeDtypeStruct((nb, rows, dim), F32),
        scratch_shapes=[pltpu.VMEM((nb, 2 * n, dim), BF16), pltpu.VMEM((nb, 2 * n, dim), BF16),
                        pltpu.VMEM((2, rows, dim), BF16), pltpu.VMEM((2, rows, dim), F32), pltpu.VMEM((rows, LANES), BF16)],
        compiler_params=pltpu.CompilerParams(vmem_limit_bytes=VMEM_LIMIT),
        name='dec_local',
    )(q_loc, zn, norm_query, norm_mlp, dec_wq, dec_wkv, dec_wo, dec_mlp, dec_out)


def solution(mesh):
    seq_spec = P('dp', ('tp', 'sp'), None)
    replicated = P()
    in_specs = (seq_spec, seq_spec, replicated, replicated, replicated, replicated, replicated, replicated, replicated, replicated,
                P(None, None, None, 'tp', None), P(None, 'tp', None, None), P(None, None, 'tp'), P(None, 'tp', None),
                replicated, replicated, replicated, replicated, replicated)

    def device_step(x_loc, q_loc, latents, norm_in, norm_query, norm_lat, enc_wq, enc_wkv, enc_wo, enc_mlp,
                    lat_wqkv, lat_wo, lat_w1, lat_w2, dec_wq, dec_wkv, dec_wo, dec_mlp, dec_out):
        layers, dim = lat_wqkv.shape[0], latents.shape[1]
        wqkv = lat_wqkv.transpose(0, 2, 3, 1, 4)
        lwo = lat_wo.reshape(layers, -1, dim)
        num, stats = encoder_local(x_loc, norm_in, latents, norm_lat[0], enc_wq, enc_wkv)
        zn = latent_all(num, stats, latents, norm_lat, enc_wkv, enc_wo, enc_mlp, wqkv, lwo, lat_w1, lat_w2)
        return decoder(q_loc, zn, norm_query, norm_lat[7], dec_wq, dec_wkv, dec_wo, dec_mlp, dec_out)

    return jax.shard_map(device_step, mesh=mesh, in_specs=in_specs, out_specs=seq_spec, check_vma=False)
```

```python
import functools
import math
import jax
import jax.numpy as jnp
from jax import lax
from jax.experimental import pallas as pl
from jax.experimental.pallas import tpu as pltpu
from jax.sharding import PartitionSpec as P

LN_EPS = 1e-5
F32, BF16 = jnp.float32, jnp.bfloat16
MESH = pl.DeviceIdType.MESH
VMEM_LIMIT = 63 * 1024 * 1024
LANES = 128
NLINE = 4
RBLK = 128
OUT_STEP = 2
ENC_STEP = 4
NCH = 4
GELU_C = math.sqrt(2.0 / math.pi)


def layer_norm(values, gain, bias):
    row_mean = jnp.mean(values, axis=-1, keepdims=True)
    centered = values - row_mean
    row_var = jnp.mean(centered * centered, axis=-1, keepdims=True)
    return (centered * lax.rsqrt(row_var + LN_EPS) * gain + bias).astype(BF16)


def gelu(x):
    return 0.5 * x * (1.0 + jnp.tanh(GELU_C * (x + 0.044715 * (x * x * x))))


def dot(a, b):
    return jnp.dot(a, b, preferred_element_type=F32)


def dot_t(a, b):
    return lax.dot_general(a, b, (((1,), (1,)), ((), ())), preferred_element_type=F32)


def split_bf16(x):
    high = x.astype(BF16)
    return high, (x - high.astype(F32)).astype(BF16)


def encoder_kernel(x_ref, nin_ref, lat_ref, nq_ref, wq_ref, wk_ref, num_ref, st_ref, qk_s, stats_s):
    b = pl.program_id(0)
    n = lat_ref.shape[0]
    dim = lat_ref.shape[1]

    @pl.when(b == 0)
    def _():
        q = dot(layer_norm(lat_ref[...].astype(F32), nq_ref[0:1, :], nq_ref[1:2, :]), wq_ref[...]).astype(BF16)
        high, low = split_bf16(dot_t(q, wk_ref[0]))
        qk_s[0:n, :] = high
        qk_s[n:2 * n, :] = low
        stats_s[...] = jnp.zeros_like(stats_s)

    each = range(x_ref.shape[0])
    xns = [layer_norm(x_ref[j].astype(F32), nin_ref[0:1, :], nin_ref[1:2, :]) for j in each]
    both = [dot_t(qk_s[...], xn) for xn in xns]
    scores = [(v[:n] + v[n:]) * (1.0 / math.sqrt(dim)) for v in both]
    maxima = [jnp.max(v, axis=1, keepdims=True) for v in scores]
    weights = [jnp.exp(v - m) for v, m in zip(scores, maxima)]
    sums = [jnp.sum(v, axis=1, keepdims=True) for v in weights]
    for j in each:
        num_ref[j] = dot(weights[j].astype(BF16), xns[j])
        here = lax.broadcasted_iota(jnp.int32, (n, LANES), 1) == b * x_ref.shape[0] + j
        stats_s[0:n, :] = jnp.where(here, maxima[j], stats_s[0:n, :])
        stats_s[n:2 * n, :] = jnp.where(here, sums[j], stats_s[n:2 * n, :])

    @pl.when(b == pl.num_programs(0) - 1)
    def _():
        st_ref[...] = stats_s[...].T[0:st_ref.shape[0], :]


def encoder_local(x_loc, norm_in, latents, norm_q, enc_wq, enc_wkv):
    nb, rows, dim = x_loc.shape
    n = latents.shape[0]
    whole = lambda shape: pl.BlockSpec(shape, lambda b: (0,) * len(shape))
    return pl.pallas_call(
        encoder_kernel,
        grid=(nb // ENC_STEP,),
        in_specs=[pl.BlockSpec((ENC_STEP, rows, dim), lambda b: (b, 0, 0)), whole((2, dim)), whole((n, dim)), whole((2, dim)),
                  whole((dim, dim)), pl.BlockSpec((1, dim, dim), lambda b: (0, 0, 0))],
        out_specs=[pl.BlockSpec((ENC_STEP, n, dim), lambda b: (b, 0, 0)), whole((nb, LANES))],
        out_shape=[jax.ShapeDtypeStruct((nb, n, dim), F32), jax.ShapeDtypeStruct((nb, LANES), F32)],
        scratch_shapes=[pltpu.VMEM((2 * n, dim), BF16), pltpu.VMEM((LANES, LANES), F32)],
        compiler_params=pltpu.CompilerParams(vmem_limit_bytes=VMEM_LIMIT),
        name='enc_local',
    )(x_loc, norm_in, latents, norm_q, enc_wq, enc_wkv)


def latent_kernel(num_ref, st_ref, lat_ref, nlat_ref, nq_ref, wkv_h, wo_h, emlp_h, qkv_h, lwo_h, lw1_h, lw2_h,
                  q_h, dwq_h, dwkv_h, dwo_h, dmlp_h, out_h,
                  wv, wo, emlp, wqkv, lwo, lw1, lw2, wsem, wkq, wvo,
                  kq_s, vo_s, xu_s, u_s, p_s, qbuf, ubuf, qsem, usem,
                  st_all, gs, d2d, ysend, yrecv, zsum, rz_a, rz_b, ln_n, ln_f, ac_n, ac_f, zown, zall,
                  s_st, r_st, s_d2, r_d2, s_y, r_y, s_za, s_zb, r_za, r_zb,
                  s_lnn, s_lnf, s_acn, s_acf, r_lnn, r_lnf, r_acn, r_acf, r_ag, s_agz, s_agc, s_agy):
    n, dim = lat_ref.shape
    rows = n // NCH
    x = lax.axis_index('dp')
    t = lax.axis_index('tp')
    sp = lax.axis_index('sp')
    y = lax.div(sp, 2)
    c = lax.rem(sp, 2)
    me = t * 4 + sp
    upper = lax.div(t, 2)
    is_end = jnp.logical_or(t == 0, t == NLINE - 1)
    is_mid = jnp.logical_not(is_end)
    e_near = upper
    e_far = 1 - upper
    inward = (x, jnp.where(t == 0, 1, jnp.where(t == 1, 2, jnp.where(t == 2, 1, 2))), sp)
    outward = (x, jnp.where(t <= 1, 0, NLINE - 1), sp)
    core_peer = (x, t, y * 2 + (1 - c))
    y_peer = (x, t, (1 - y) * 2 + c)

    def rc(src, dst, ssem, rsem, dev):
        return pltpu.make_async_remote_copy(src_ref=src, dst_ref=dst, send_sem=ssem, recv_sem=rsem,
                                            device_id=dev, device_id_type=MESH)

    def peer(p):
        g = lax.rem(me + p, 16)
        return g, (x, lax.div(g, 4), lax.rem(g, 4))

    def fetch(first, pairs):
        copies = [pltpu.make_async_copy(src, dst, wsem.at[first + k]) for k, (src, dst) in enumerate(pairs)]
        for copy in copies:
            copy.start()
        return copies

    dec_loads = fetch(0, ((dwkv_h, emlp), (dwq_h, wv), (dwo_h, wo)))
    lat_loads = fetch(3, ((qkv_h, wqkv), (lwo_h, lwo), (lw1_h, lw1), (lw2_h, lw2)))

    barrier = pltpu.get_barrier_semaphore()

    def greet(p, carry):
        pl.semaphore_signal(barrier, inc=1, device_id=peer(p)[1], device_id_type=MESH)
        return carry

    lax.fori_loop(1, 16, greet, 0)
    pl.semaphore_wait(barrier, 15)

    def send_stats(p, carry):
        g, dev = peer(p)
        rc(st_ref, st_all.at[me], s_st.at[g], r_st.at[me], dev).start()
        return carry

    lax.fori_loop(1, 16, send_stats, 0)

    def core_copy(i, yb):
        return rc(num_ref.at[pl.ds(yb * 8 + (1 - c) * 4 + i * 2, 2)], d2d.at[i, yb], s_d2.at[i, yb], r_d2.at[i, yb], core_peer)

    for i in range(2):
        core_copy(i, 1 - y).start()
        core_copy(i, y).start()
    st_all[me] = st_ref[...]

    def wait_stats(p, carry):
        g, dev = peer(p)
        rc(st_ref, st_all.at[g], s_st.at[g], r_st.at[g], dev).wait_recv()
        return carry

    lax.fori_loop(1, 16, wait_stats, 0)
    top = lax.fori_loop(1, 16, lambda d, m: jnp.maximum(m, st_all[d]), st_all[0])

    def add_sum(d, total):
        stats = st_all[d]
        return total + jnp.exp(stats - top) * pltpu.roll(stats, n, 1)

    total = lax.fori_loop(0, 16, add_sum, jnp.zeros_like(top))
    partner = t * 4 + y * 2 + (1 - c)
    gs[...] = jnp.zeros_like(gs)
    gs[0:16, :] = jnp.exp(st_all[me] - top) / total
    scale_own = gs[...].T[0:n, :]
    gs[0:16, :] = jnp.exp(st_all[partner] - top) / total
    scale_peer = gs[...].T[0:n, :]
    gs[0:n, :] = scale_own
    gs[n:2 * n, :] = scale_peer
    lane = lax.broadcasted_iota(jnp.int32, (2 * n, LANES), 1)

    def y_copy(i, e):
        return rc(ysend.at[i, e], yrecv.at[i, e], s_y.at[i, e], r_y.at[i, e], y_peer)

    def scaled(i, yb, e):
        b = yb * 8 + c * 4 + i * 2 + e
        col = jnp.sum(jnp.where(lane == b, gs[...], 0.0), axis=1, keepdims=True)
        return col[0:n] * num_ref[b] + col[n:2 * n] * d2d[i, yb, e]

    def scale_step(i, carry):
        core_copy(i, 1 - y).wait_recv()
        for e in range(2):
            ysend[i, e] = scaled(i, 1 - y, e)
            y_copy(i, e).start()
        core_copy(i, y).wait_recv()
        for e in range(2):
            zsum[i, e] = scaled(i, y, e)
        return carry

    lax.fori_loop(0, 2, scale_step, 0)

    def y_add(i):
        for e in range(2):
            y_copy(i, e).wait_recv()
            zsum[i, e] = zsum[i, e] + yrecv[i, e]

    def chunk(ch):
        return pl.ds(pl.multiple_of(ch * rows, rows), rows)

    def z_end_send(i):
        def step(ch, carry):
            rc(zsum.at[i, e_far, chunk(ch)], rz_a.at[i, chunk(ch)], s_za.at[i, ch], r_za.at[i, ch], inward).start()
            return carry
        lax.fori_loop(0, NCH, step, 0)

    def z_mid(i):
        def near(ch, carry):
            cp = rc(rz_a.at[i, chunk(ch)], rz_b.at[i, chunk(ch)], s_za.at[i, ch], r_zb.at[i, ch], inward)
            rc(rz_a.at[i, chunk(ch)], rz_a.at[i, chunk(ch)], s_za.at[i, ch], r_za.at[i, ch], outward).wait_recv()
            rz_a[i, chunk(ch)] = rz_a[i, chunk(ch)] + zsum[i, e_far, chunk(ch)]
            cp.start()
            return carry

        def far(ch, carry):
            cp = rc(rz_b.at[i, chunk(ch)], rz_b.at[i, chunk(ch)], s_zb.at[i, ch], r_zb.at[i, ch], outward)
            cp.wait_recv()
            rz_b[i, chunk(ch)] = rz_b[i, chunk(ch)] + zsum[i, e_near, chunk(ch)]
            cp.start()
            return carry

        lax.fori_loop(0, NCH, near, 0)
        lax.fori_loop(0, NCH, far, 0)

    def z_end_recv(i):
        def step(ch, carry):
            rc(rz_b.at[i, chunk(ch)], rz_b.at[i, chunk(ch)], s_zb.at[i, ch], r_zb.at[i, ch], inward).wait_recv()
            return carry
        lax.fori_loop(0, NCH, step, 0)
        return rz_b[i] + zsum[i, e_near]

    def norm(index, values):
        return layer_norm(values, nlat_ref[index, 0:1, :], nlat_ref[index, 1:2, :])

    def attention(layer, xn):
        hd = wqkv.shape[4]
        qkv = [dot(xn, jnp.concatenate([wqkv[layer, j, 0], wqkv[layer, j, 1]], axis=1)).astype(BF16) for j in range(3)]
        outs = []
        for h in range(2):
            q, k, v = (part[:, h * hd:(h + 1) * hd] for part in qkv)
            scores = dot_t(q, k) * (1.0 / math.sqrt(hd))
            weights = jnp.exp(scores - jnp.max(scores, axis=1, keepdims=True))
            probs = (weights / jnp.sum(weights, axis=1, keepdims=True)).astype(BF16)
            outs.append(dot(probs, v).astype(BF16))
        return dot(jnp.concatenate(outs, axis=1), lwo[layer])

    def mlp(layer, xn):
        return dot(gelu(dot(xn, lw1[layer])).astype(BF16), lw2[layer])

    kinds = (attention, mlp)

    def ln_near(u, ch):
        return ln_n.at[u, chunk(ch)]

    def source(kind, layer, u, s):
        values = zown[s]
        xn = norm(2 + 2 * layer + kind, values)
        ln_n[u] = xn.astype(F32)

        def send_ln(ch, carry):
            rc(ln_n.at[u, chunk(ch)], ln_n.at[u, chunk(ch)], s_lnn.at[u, ch], r_lnn.at[u, ch], inward).start()
            return carry

        lax.fori_loop(0, NCH, send_ln, 0)
        ac_n[u] = values + kinds[kind](layer, xn)

        def send_ac(ch, carry):
            rc(ac_n.at[u, chunk(ch)], ac_n.at[u, chunk(ch)], s_acn.at[u, ch], r_acn.at[u, ch], inward).start()
            return carry

        lax.fori_loop(0, NCH, send_ac, 0)

    def sink(kind, layer, u, s):
        def wait_ln(ch, carry):
            rc(ln_f.at[u, chunk(ch)], ln_f.at[u, chunk(ch)], s_lnf.at[u, ch], r_lnf.at[u, ch], inward).wait_recv()
            return carry

        lax.fori_loop(0, NCH, wait_ln, 0)
        part = kinds[kind](layer, ln_f[u].astype(BF16))

        def wait_ac(ch, carry):
            rc(ac_f.at[u, chunk(ch)], ac_f.at[u, chunk(ch)], s_acf.at[u, ch], r_acf.at[u, ch], inward).wait_recv()
            return carry

        lax.fori_loop(0, NCH, wait_ac, 0)
        zown[s] = ac_f[u] + part

    def middle(kind, layer, u):
        def near_ln(ch, carry):
            rc(ln_n.at[u, chunk(ch)], ln_n.at[u, chunk(ch)], s_lnn.at[u, ch], r_lnn.at[u, ch], outward).wait_recv()
            rc(ln_n.at[u, chunk(ch)], ln_f.at[u, chunk(ch)], s_lnn.at[u, ch], r_lnf.at[u, ch], inward).start()
            return carry

        lax.fori_loop(0, NCH, near_ln, 0)
        zown[0] = kinds[kind](layer, ln_n[u].astype(BF16))

        def both(ch, carry):
            cp = rc(ln_f.at[u, chunk(ch)], ln_f.at[u, chunk(ch)], s_lnf.at[u, ch], r_lnf.at[u, ch], outward)
            cp.wait_recv()
            cp.start()
            rc(ac_n.at[u, chunk(ch)], ac_n.at[u, chunk(ch)], s_acn.at[u, ch], r_acn.at[u, ch], outward).wait_recv()
            ac_n[u, chunk(ch)] = ac_n[u, chunk(ch)] + zown[0, chunk(ch)]
            rc(ac_n.at[u, chunk(ch)], ac_f.at[u, chunk(ch)], s_acn.at[u, ch], r_acf.at[u, ch], inward).start()
            return carry

        lax.fori_loop(0, NCH, both, 0)
        zown[1] = kinds[kind](layer, ln_f[u].astype(BF16))
        if kind == 1:
            @pl.when(u == 7)
            def _():
                ag_relay(0, e_near, inward)

        def far_ac(ch, carry):
            cp = rc(ac_f.at[u, chunk(ch)], ac_f.at[u, chunk(ch)], s_acf.at[u, ch], r_acf.at[u, ch], outward)
            cp.wait_recv()
            ac_f[u, chunk(ch)] = ac_f[u, chunk(ch)] + zown[1, chunk(ch)]
            cp.start()
            return carry

        lax.fori_loop(0, NCH, far_ac, 0)

    def line_seq(i, e):
        return y * 8 + c * 4 + i * 2 + e

    def ag_copy(b, ch, sems, dev):
        return rc(zall.at[b, chunk(ch)], zall.at[b, chunk(ch)], sems.at[b, ch], r_ag.at[b, ch], dev)

    def ag_send(b, ch, z_dev):
        if z_dev is not None:
            ag_copy(b, ch, s_agz, z_dev).start()
        ag_copy(b, ch, s_agy, y_peer).start()
        ag_copy(b, ch, s_agc, core_peer).start()

    def ag_source(i):
        b = line_seq(i, e_near)
        zall[b] = norm(6, zown[i]).astype(F32)

        def step(ch, carry):
            ag_send(b, ch, inward)
            return carry

        lax.fori_loop(0, NCH, step, 0)

    def ag_relay(i, e, z_dev):
        b = line_seq(i, e)

        def step(ch, carry):
            ag_copy(b, ch, s_agz, inward).wait_recv()
            ag_send(b, ch, z_dev)
            return carry

        lax.fori_loop(0, NCH, step, 0)

    def ag_cross(i, e):
        b = (1 - y) * 8 + c * 4 + i * 2 + e

        def step(ch, carry):
            ag_copy(b, ch, s_agy, y_peer).wait_recv()
            ag_copy(b, ch, s_agc, core_peer).start()
            return carry

        lax.fori_loop(0, NCH, step, 0)

    for load in dec_loads:
        load.wait()

    def products(k, carry):
        part = pl.ds(pl.multiple_of(k * 256, 256), 256)
        wkq[part] = dot_t(emlp[0, part], wv[...]).astype(BF16)
        wvo[part] = dot(emlp[1, part], wo[...]).astype(BF16)
        return carry

    lax.fori_loop(0, dim // 256, products, 0)
    enc_loads = fetch(7, ((wkv_h.at[1], wv), (wo_h, wo), (emlp_h, emlp)))
    def tail_loads():
        return [pltpu.make_async_copy(dmlp_h, emlp, wsem.at[10])]

    y_add(0)

    @pl.when(is_end)
    def _():
        z_end_send(0)

    @pl.when(is_mid)
    def _():
        z_mid(0)

    y_add(1)
    for load in lat_loads + enc_loads:
        load.wait()

    @pl.when(is_end)
    def _():
        z_end_send(1)

        def start(s, carry):
            both = jnp.concatenate(split_bf16(z_end_recv(s)), axis=0)
            both = dot(both, wv[...])
            attended = (both[0:n] + both[n:2 * n]).astype(BF16)
            z = lat_ref[...].astype(F32) + dot(attended, wo[...])
            zown[s] = z + dot(gelu(dot(norm(1, z), emlp[0])).astype(BF16), emlp[1])
            source(0, 0, s, s)
            return carry

        lax.fori_loop(0, 2, start, 0)
        for load in tail_loads():
            load.start()

        def layer_step(layer, carry):
            def attn_unit(s, inner):
                u = layer * 4 + s
                sink(0, layer, u, s)
                source(1, layer, u + 2, s)
                return inner

            lax.fori_loop(0, 2, attn_unit, 0)

            def mlp_unit(s, inner):
                u = layer * 4 + 2 + s
                sink(1, layer, u, s)

                @pl.when(layer == 0)
                def _():
                    source(0, 1, u + 2, s)

                @pl.when(layer == 1)
                def _():
                    ag_source(s)

                return inner

            lax.fori_loop(0, 2, mlp_unit, 0)
            return carry

        lax.fori_loop(0, 2, layer_step, 0)

    @pl.when(is_mid)
    def _():
        z_mid(1)
        for load in tail_loads():
            load.start()

        def layer_step(layer, carry):
            for kind in range(2):
                def unit(s, inner):
                    middle(kind, layer, layer * 4 + 2 * kind + s)
                    return inner
                lax.fori_loop(0, 2, unit, 0)
            return carry

        lax.fori_loop(0, 2, layer_step, 0)

    def order(k):
        i = lax.div(k, 8)
        r = lax.rem(k, 8)
        pair = lax.div(r, 2)
        odd = lax.rem(pair, 2)
        yb = y + odd - 2 * y * odd
        core = lax.rem(r, 2)
        cb = c + core - 2 * c * core
        far = lax.div(pair, 2)
        e = e_near + far - 2 * e_near * far
        return yb * 8 + cb * 4 + i * 2 + e

    def q_copy(k):
        return pltpu.make_async_copy(q_h.at[order(k)], qbuf.at[lax.rem(k, 2)], qsem.at[lax.rem(k, 2)])

    def u_copy(k):
        return pltpu.make_async_copy(ubuf.at[lax.rem(k, 2)], out_h.at[order(k)], usem.at[lax.rem(k, 2)])

    q_copy(0).start()
    for load in tail_loads():
        load.wait()
    xu_s[...] = jnp.zeros_like(xu_s)
    u_s[...] = jnp.zeros_like(u_s)
    nrow = qbuf.shape[1]
    nblk = nrow // RBLK
    cblk = dim // nblk

    def decode(k, carry):
        @pl.when(jnp.logical_and(lax.rem(k, 2) == 0, k < 16))
        def _():
            other = order(k + 1)

            def step(ch, inner):
                ag_copy(other, ch, s_agc, core_peer).wait_recv()
                return inner

            lax.fori_loop(0, NCH, step, 0)
            zn = jnp.concatenate([zall[order(k)], zall[other]], axis=0).astype(BF16)
            for weights, target in ((wkq, kq_s), (wvo, vo_s)):
                high, low = split_bf16(dot(zn, weights[...]))
                for j in range(2):
                    target[j, 0:n, :] = high[j * n:(j + 1) * n]
                    target[j, n:2 * n, :] = low[j * n:(j + 1) * n]

        @pl.when(k < 16)
        def _():
            q_copy(k).wait()

        @pl.when(k < 15)
        def _():
            q_copy(k + 1).start()

        @pl.when(k >= 3)
        def _():
            u_copy(k - 3).wait()

        ahead = lax.rem(k, 2)
        now = 1 - ahead
        xu = xu_s[now]
        hidden = []
        for blk in range(nblk):
            part = pl.ds(blk * RBLK, RBLK)
            cols = slice(blk * cblk, (blk + 1) * cblk)
            hidden.append(gelu(dot(xu, emlp[0, :, cols])).astype(BF16))
            xq = layer_norm(qbuf[ahead, part].astype(F32), nq_ref[0:1, :], nq_ref[1:2, :])
            both = dot_t(xq, kq_s[ahead])
            scores = (both + pltpu.roll(both, n, 1)) * (1.0 / math.sqrt(dim))
            weights = jnp.exp(scores - jnp.max(scores, axis=1, keepdims=True))
            p_s[part] = (weights / (0.5 * jnp.sum(weights, axis=1, keepdims=True))).astype(BF16)
        hidden = jnp.concatenate(hidden, axis=1)
        for blk in range(nblk):
            part = pl.ds(blk * RBLK, RBLK)
            cols = slice(blk * cblk, (blk + 1) * cblk)
            ubuf[now, :, cols] = (u_s[now, :, cols] + dot(hidden, emlp[1, :, cols])).astype(BF16)
            u = dot(p_s[part], vo_s[ahead])
            u_s[ahead, part] = u
            xu_s[ahead, part] = norm(7, u)

        @pl.when(k >= 1)
        def _():
            u_copy(k - 1).start()

        def far_relay(i):
            @pl.when(is_mid)
            def _():
                ag_relay(i, e_far, outward)

            @pl.when(is_end)
            def _():
                ag_relay(i, e_far, None)

        def near_relay(i):
            @pl.when(is_mid)
            def _():
                ag_relay(i, e_near, inward)

        for when, what in ((0, lambda: far_relay(0)), (1, lambda: ag_cross(0, e_near)), (3, lambda: ag_cross(0, e_far)),
                           (4, lambda: near_relay(1)), (6, lambda: far_relay(1)), (7, lambda: ag_cross(1, e_near)),
                           (9, lambda: ag_cross(1, e_far))):
            pl.when(k == when)(what)
        return carry

    lax.fori_loop(0, 17, decode, 0)
    u_copy(14).wait()
    u_copy(15).wait()

    def done_stats(p, carry):
        g, dev = peer(p)
        rc(st_ref, st_all.at[me], s_st.at[g], r_st.at[me], dev).wait_send()
        return carry

    lax.fori_loop(1, 16, done_stats, 0)
    for i in range(2):
        core_copy(i, 1 - y).wait_send()
        core_copy(i, y).wait_send()
        for e in range(2):
            y_copy(i, e).wait_send()

    def done_z(i, carry):
        def step(ch, inner):
            rc(rz_a.at[i, chunk(ch)], rz_a.at[i, chunk(ch)], s_za.at[i, ch], r_za.at[i, ch], inward).wait_send()

            @pl.when(is_mid)
            def _():
                rc(rz_b.at[i, chunk(ch)], rz_b.at[i, chunk(ch)], s_zb.at[i, ch], r_zb.at[i, ch], outward).wait_send()

            return inner

        lax.fori_loop(0, NCH, step, 0)
        return carry

    lax.fori_loop(0, 2, done_z, 0)

    def done_units(u, carry):
        def step(ch, inner):
            rc(ln_n.at[u, chunk(ch)], ln_n.at[u, chunk(ch)], s_lnn.at[u, ch], r_lnn.at[u, ch], inward).wait_send()
            rc(ac_n.at[u, chunk(ch)], ac_n.at[u, chunk(ch)], s_acn.at[u, ch], r_acn.at[u, ch], inward).wait_send()

            @pl.when(is_mid)
            def _():
                rc(ln_f.at[u, chunk(ch)], ln_f.at[u, chunk(ch)], s_lnf.at[u, ch], r_lnf.at[u, ch], outward).wait_send()
                rc(ac_f.at[u, chunk(ch)], ac_f.at[u, chunk(ch)], s_acf.at[u, ch], r_acf.at[u, ch], outward).wait_send()

            return inner

        lax.fori_loop(0, NCH, step, 0)
        return carry

    lax.fori_loop(0, 8, done_units, 0)

    def done_ag(i, carry):
        for e in range(2):
            b = line_seq(i, e)
            other = (1 - y) * 8 + c * 4 + i * 2 + e

            def step(ch, inner):
                ag_copy(b, ch, s_agy, y_peer).wait_send()
                ag_copy(b, ch, s_agc, core_peer).wait_send()
                ag_copy(other, ch, s_agc, core_peer).wait_send()

                @pl.when(jnp.logical_or(is_mid, e == e_near))
                def _():
                    ag_copy(b, ch, s_agz, inward).wait_send()

                return inner

            lax.fori_loop(0, NCH, step, 0)
        return carry

    lax.fori_loop(0, 2, done_ag, 0)


def latent_all(num, stats, q_loc, latents, norm_lat, norm_query, enc_wkv, enc_wo, enc_mlp, wqkv, lwo, lw1, lw2,
               dec_wq, dec_wkv, dec_wo, dec_mlp):
    nb, n, dim = num.shape
    rows = q_loc.shape[1]
    vm = pl.BlockSpec(memory_space=pltpu.VMEM)
    hbm = pl.BlockSpec(memory_space=pl.ANY)
    dma = pltpu.SemaphoreType.DMA
    buf = lambda *shape: pltpu.VMEM(shape + (n, dim), F32)
    half = lambda *shape: pltpu.VMEM(shape + (dim,), BF16)
    return pl.pallas_call(
        latent_kernel,
        in_specs=[vm] * 5 + [hbm] * 12,
        out_specs=hbm,
        out_shape=jax.ShapeDtypeStruct((nb, rows, dim), BF16),
        scratch_shapes=[
            half(dim), half(dim), pltpu.VMEM(enc_mlp.shape, BF16),
            pltpu.VMEM(wqkv.shape, BF16), pltpu.VMEM(lwo.shape, BF16), pltpu.VMEM(lw1.shape, BF16), pltpu.VMEM(lw2.shape, BF16),
            dma((11,)), half(dim), half(dim),
            half(2, 2 * n), half(2, 2 * n), half(2, rows), pltpu.VMEM((2, rows, dim), F32), pltpu.VMEM((rows, LANES), BF16),
            half(2, rows), half(2, rows), dma((2,)), dma((2,)),
            pltpu.VMEM((16, nb, LANES), F32), pltpu.VMEM((LANES, LANES), F32),
            buf(2, 2, 2), buf(2, 2), buf(2, 2), buf(2, 2), buf(2), buf(2),
            buf(8), buf(8), buf(8), buf(8), buf(2), buf(nb),
            dma((16,)), dma((16,)), dma((2, 2)), dma((2, 2)), dma((2, 2)), dma((2, 2)),
            dma((2, NCH)), dma((2, NCH)), dma((2, NCH)), dma((2, NCH)),
        ] + [dma((8, NCH))] * 8 + [dma((nb, NCH))] * 4,
        compiler_params=pltpu.CompilerParams(vmem_limit_bytes=VMEM_LIMIT, collective_id=0, has_side_effects=True),
        name='latent_all',
    )(num, stats, latents, norm_lat, norm_query, enc_wkv, enc_wo, enc_mlp, wqkv, lwo, lw1, lw2,
      q_loc, dec_wq, dec_wkv, dec_wo, dec_mlp)


def out_kernel(u_ref, w_ref, y_ref):
    for j in range(u_ref.shape[0]):
        y_ref[j] = dot(u_ref[j], w_ref[...])


def out_product(u, dec_out):
    nb, rows, dim = u.shape
    return pl.pallas_call(
        out_kernel,
        grid=(nb // OUT_STEP,),
        in_specs=[pl.BlockSpec((OUT_STEP, rows, dim), lambda b: (b, 0, 0)), pl.BlockSpec((dim, dim), lambda b: (0, 0))],
        out_specs=pl.BlockSpec((OUT_STEP, rows, dim), lambda b: (b, 0, 0)),
        out_shape=jax.ShapeDtypeStruct((nb, rows, dim), F32),
        compiler_params=pltpu.CompilerParams(vmem_limit_bytes=VMEM_LIMIT),
        name='out_product',
    )(u, dec_out)


def solution(mesh):
    seq_spec = P('dp', ('tp', 'sp'), None)
    replicated = P()
    in_specs = (seq_spec, seq_spec, replicated, replicated, replicated, replicated, replicated, replicated, replicated, replicated,
                P(None, None, None, 'tp', None), P(None, 'tp', None, None), P(None, None, 'tp'), P(None, 'tp', None),
                replicated, replicated, replicated, replicated, replicated)

    def device_step(x_loc, q_loc, latents, norm_in, norm_query, norm_lat, enc_wq, enc_wkv, enc_wo, enc_mlp,
                    lat_wqkv, lat_wo, lat_w1, lat_w2, dec_wq, dec_wkv, dec_wo, dec_mlp, dec_out):
        layers, dim = lat_wqkv.shape[0], latents.shape[1]
        wqkv = lat_wqkv.transpose(0, 2, 3, 1, 4)
        lwo = lat_wo.reshape(layers, -1, dim)
        num, stats = encoder_local(x_loc, norm_in, latents, norm_lat[0], enc_wq, enc_wkv)
        u = latent_all(num, stats, q_loc, latents, norm_lat, norm_query, enc_wkv, enc_wo, enc_mlp, wqkv, lwo, lat_w1, lat_w2,
                       dec_wq, dec_wkv, dec_wo, dec_mlp)
        return out_product(u, dec_out)

    return jax.shard_map(device_step, mesh=mesh, in_specs=in_specs, out_specs=seq_spec, check_vma=False)
```

```python
import functools
import math
import jax
import jax.numpy as jnp
from jax import lax
from jax.experimental import pallas as pl
from jax.experimental.pallas import tpu as pltpu
from jax.sharding import PartitionSpec as P

LN_EPS = 1e-5
F32, BF16 = jnp.float32, jnp.bfloat16
MESH = pl.DeviceIdType.MESH
VMEM_LIMIT = 63 * 1024 * 1024
LANES = 128
NLINE = 4
RBLK = 128
CBLK = 256
OUT_STEP = 4
PAIR_AT = 4
NCH = 4
GELU_C = math.sqrt(2.0 / math.pi)


def layer_norm(values, gain, bias):
    row_mean = jnp.mean(values, axis=-1, keepdims=True)
    centered = values - row_mean
    row_var = jnp.mean(centered * centered, axis=-1, keepdims=True)
    return (centered * lax.rsqrt(row_var + LN_EPS) * gain + bias).astype(BF16)


def gelu(x):
    return 0.5 * x * (1.0 + jnp.tanh(GELU_C * (x + 0.044715 * (x * x * x))))


def repeat(count, step):
    lax.fori_loop(0, count, step, 0)


def each_peer(step):
    lax.fori_loop(1, 16, step, 0)


def dot(a, b):
    return jnp.dot(a, b, preferred_element_type=F32)


def dot_t(a, b):
    return lax.dot_general(a, b, (((1,), (1,)), ((), ())), preferred_element_type=F32)


def split_bf16(x):
    high = x.astype(BF16)
    return high, (x - high.astype(F32)).astype(BF16)


def latent_kernel(nin_ref, lat_ref, nlat_ref, nq_ref, x_h, ewq_h, wkv_h, wo_h, emlp_h, qkv_h, lwo_h, lw1_h, lw2_h,
                  q_h, dwq_h, dwkv_h, dwo_h, dmlp_h, dout_h, out_h, p_h, voo_h, w2o_h,
                  wv, wo, emlp, wqkv, lwo, lw1, lw2, wsem, wkq, wvo, wvoo, w2o,
                  kq_s, vo_s, voo_s, xq_s, xu0, xu1, p0, p1, q0, q1, h0, h1, xbuf, qsem, usem, psem, vsem, xsem,
                  num, qk_s, stats_s, st_mine,
                  st_all, gs, d2d, ysend, yrecv, zsum, rz_a, rz_b, ln_n, ln_f, ac_n, ac_f, zown, zall,
                  s_st, r_st, s_d2, r_d2, s_y, r_y, s_za, s_zb, r_za, r_zb,
                  s_lnn, s_lnf, s_acn, s_acf, r_lnn, r_lnf, r_acn, r_acf, r_ag, s_agz, s_agc, s_agy):
    n, dim = lat_ref.shape
    rows = n // NCH
    x = lax.axis_index('dp')
    t = lax.axis_index('tp')
    sp = lax.axis_index('sp')
    y = lax.div(sp, 2)
    c = lax.rem(sp, 2)
    me = t * 4 + sp
    upper = lax.div(t, 2)
    is_end = jnp.logical_or(t == 0, t == NLINE - 1)
    is_mid = jnp.logical_not(is_end)
    e_near = upper
    e_far = 1 - upper
    inward = (x, jnp.where(t == 0, 1, jnp.where(t == 1, 2, jnp.where(t == 2, 1, 2))), sp)
    outward = (x, jnp.where(t <= 1, 0, NLINE - 1), sp)
    core_peer = (x, t, y * 2 + (1 - c))
    y_peer = (x, t, (1 - y) * 2 + c)

    def rc(src, dst, ssem, rsem, dev):
        return pltpu.make_async_remote_copy(src_ref=src, dst_ref=dst, send_sem=ssem, recv_sem=rsem,
                                            device_id=dev, device_id_type=MESH)

    def peer(p):
        g = lax.rem(me + p, 16)
        return g, (x, lax.div(g, 4), lax.rem(g, 4))

    def fetch(first, pairs):
        copies = [pltpu.make_async_copy(src, dst, wsem.at[first + k]) for k, (src, dst) in enumerate(pairs)]
        for copy in copies:
            copy.start()
        return copies

    def x_copy(g):
        first, _, _ = group(g)
        slot = lax.rem(g, 2)
        return pltpu.make_async_copy(x_h.at[pl.ds(first, 2)], xbuf.at[pl.ds(2 * slot, 2)], xsem.at[slot])

    def group(g):
        i = lax.div(g, 4)
        j = lax.rem(g, 4)
        core = lax.div(j, 2)
        cb = 1 - c + core * (2 * c - 1)
        side = lax.rem(j, 2)
        yb = 1 - y + side * (2 * y - 1)
        return yb * 8 + cb * 4 + i * 2, i, j

    query_loads = fetch(0, ((ewq_h, wv), (wkv_h.at[0], wo)))
    x_copy(0).start()
    key_loads = fetch(2, ((dwkv_h, emlp),))
    lat_loads = fetch(3, ((qkv_h, wqkv), (lwo_h, lwo), (lw1_h, lw1)))
    out_loads = fetch(13, ((dmlp_h.at[1], lw2.at[0]), (dout_h, lw2.at[1])))

    barrier = pltpu.get_barrier_semaphore()

    def greet(p, carry):
        pl.semaphore_signal(barrier, inc=1, device_id=peer(p)[1], device_id_type=MESH)
        return carry

    each_peer(greet)

    def norm(index, values):
        return layer_norm(values, nlat_ref[index, 0:1, :], nlat_ref[index, 1:2, :])

    for load in query_loads:
        load.wait()
    q = dot(norm(0, lat_ref[...].astype(F32)), wv[...]).astype(BF16)
    high, low = split_bf16(dot_t(q, wo[...]))
    qk_s[0:n, :] = high
    qk_s[n:2 * n, :] = low
    stats_s[...] = jnp.zeros_like(stats_s)
    dec_loads = key_loads + fetch(11, ((dwq_h, wv), (dwo_h, wo)))

    def core_copy(i, yb):
        return rc(num.at[pl.ds(yb * 8 + (1 - c) * 4 + i * 2, 2)], d2d.at[i, yb], s_d2.at[i, yb], r_d2.at[i, yb], core_peer)

    def y_copy(i, e):
        return rc(ysend.at[i, e], yrecv.at[i, e], s_y.at[i, e], r_y.at[i, e], y_peer)

    def stats_copy(i, src, g, dev):
        return rc(st_mine.at[i], st_all.at[i, src], s_st.at[i, g], r_st.at[i, src], dev)

    lane = lax.broadcasted_iota(jnp.int32, (2 * n, LANES), 1)

    partner = t * 4 + y * 2 + (1 - c)

    def set_scales(first, second):
        gs[...] = jnp.zeros_like(gs)
        gs[0:16, :] = first
        upper_part = gs[...].T[0:n, :]
        gs[0:16, :] = second
        lower_part = gs[...].T[0:n, :]
        gs[0:n, :] = upper_part
        gs[n:2 * n, :] = lower_part

    def scales(b):
        col = jnp.sum(jnp.where(lane == b, gs[...], 0.0), axis=1, keepdims=True)
        return col[0:n], col[n:2 * n]

    def pair_step(i):
        stats_copy(i, partner, partner, core_peer).wait_recv()
        mine, other = st_all[i, me], st_all[i, partner]
        top = jnp.maximum(mine, other)
        set_scales(jnp.exp(mine - top), jnp.exp(other - top))
        for side in range(2):
            yb = y if side else 1 - y
            core_copy(i, yb).wait_recv()
            for e in range(2):
                b = yb * 8 + c * 4 + i * 2 + e
                first, second = scales(b)
                value = first * num[b] + second * d2d[i, yb, e]
                if side:
                    zsum[i, e] = value
                else:
                    ysend[i, e] = value
                    y_copy(i, e).start()

    def encode(g, carry):
        first, i, j = group(g)
        x_copy(g).wait()

        @pl.when(g < 7)
        def _():
            x_copy(g + 1).start()

        slot = 2 * lax.rem(g, 2)
        each = range(2)
        xns = [layer_norm(xbuf[slot + k].astype(F32), nin_ref[0:1, :], nin_ref[1:2, :]) for k in each]
        both = [dot_t(qk_s[...], xn) for xn in xns]
        scores = [(v[:n] + v[n:]) * (1.0 / math.sqrt(dim)) for v in both]
        maxima = [jnp.max(v, axis=1, keepdims=True) for v in scores]
        weights = [jnp.exp(v - m) for v, m in zip(scores, maxima)]
        sums = [jnp.sum(v, axis=1, keepdims=True) for v in weights]
        for k in each:
            num[first + k] = dot(weights[k].astype(BF16), xns[k])
            here = lax.broadcasted_iota(jnp.int32, (n, LANES), 1) == first + k
            stats_s[0:n, :] = jnp.where(here, maxima[k], stats_s[0:n, :])
            stats_s[n:2 * n, :] = jnp.where(here, sums[k], stats_s[n:2 * n, :])

        @pl.when(j == 1)
        def _():
            core_copy(i, 1 - y).start()
            core_copy(i, y).start()

        @pl.when(j == 3)
        def _():
            mine = stats_s[...].T[0:16, :]
            st_mine[i] = mine
            st_all[i, me] = mine

            def send_stats(p, inner):
                dst, dev = peer(p)
                stats_copy(i, me, dst, dev).start()
                return inner

            each_peer(send_stats)

        @pl.when(g == PAIR_AT)
        def _():
            pair_step(0)

        return carry

    pl.semaphore_wait(barrier, 15)
    repeat(8, encode)

    def y_add(i):
        def wait_stats(p, carry):
            g, dev = peer(p)

            @pl.when(g != partner)
            def _():
                stats_copy(i, g, g, dev).wait_recv()

            return carry

        each_peer(wait_stats)
        top = lax.fori_loop(1, 16, lambda d, m: jnp.maximum(m, st_all[i, d]), st_all[i, 0])

        def add_sum(d, total):
            stats = st_all[i, d]
            return total + jnp.exp(stats - top) * pltpu.roll(stats, n, 1)

        total = lax.fori_loop(0, 16, add_sum, jnp.zeros_like(top))
        across = t * 4 + (1 - y) * 2
        here = jnp.maximum(st_all[i, me], st_all[i, partner])
        there = jnp.maximum(st_all[i, across], st_all[i, across + 1])
        set_scales(jnp.exp(here - top) / total, jnp.exp(there - top) / total)
        for e in range(2):
            first, second = scales(y * 8 + c * 4 + i * 2 + e)
            y_copy(i, e).wait_recv()
            zsum[i, e] = first * zsum[i, e] + second * yrecv[i, e]

    def chunk(ch):
        return pl.ds(pl.multiple_of(ch * rows, rows), rows)

    def z_end_send(i):
        def step(ch, carry):
            rc(zsum.at[i, e_far, chunk(ch)], rz_a.at[i, chunk(ch)], s_za.at[i, ch], r_za.at[i, ch], inward).start()
            return carry
        repeat(NCH, step)

    def z_mid(i):
        def near(ch, carry):
            cp = rc(rz_a.at[i, chunk(ch)], rz_b.at[i, chunk(ch)], s_za.at[i, ch], r_zb.at[i, ch], inward)
            rc(rz_a.at[i, chunk(ch)], rz_a.at[i, chunk(ch)], s_za.at[i, ch], r_za.at[i, ch], outward).wait_recv()
            rz_a[i, chunk(ch)] = rz_a[i, chunk(ch)] + zsum[i, e_far, chunk(ch)]
            cp.start()
            return carry

        def far(ch, carry):
            cp = rc(rz_b.at[i, chunk(ch)], rz_b.at[i, chunk(ch)], s_zb.at[i, ch], r_zb.at[i, ch], outward)
            cp.wait_recv()
            rz_b[i, chunk(ch)] = rz_b[i, chunk(ch)] + zsum[i, e_near, chunk(ch)]
            cp.start()
            return carry

        repeat(NCH, near)
        repeat(NCH, far)

    def z_end_recv(i):
        def step(ch, carry):
            rc(rz_b.at[i, chunk(ch)], rz_b.at[i, chunk(ch)], s_zb.at[i, ch], r_zb.at[i, ch], inward).wait_recv()
            return carry
        repeat(NCH, step)
        return rz_b[i] + zsum[i, e_near]

    def attention(layer, xn):
        hd = wqkv.shape[4]
        qkv = [dot(xn, jnp.concatenate([wqkv[layer, j, 0], wqkv[layer, j, 1]], axis=1)).astype(BF16) for j in range(3)]
        outs = []
        for h in range(2):
            q, k, v = (part[:, h * hd:(h + 1) * hd] for part in qkv)
            scores = dot_t(q, k) * (1.0 / math.sqrt(hd))
            weights = jnp.exp(scores - jnp.max(scores, axis=1, keepdims=True))
            probs = (weights / jnp.sum(weights, axis=1, keepdims=True)).astype(BF16)
            outs.append(dot(probs, v).astype(BF16))
        return dot(jnp.concatenate(outs, axis=1), lwo[layer])

    def mlp(layer, xn):
        return dot(gelu(dot(xn, lw1[layer])).astype(BF16), lw2[layer])

    kinds = (attention, mlp)

    def ln_near(u, ch):
        return ln_n.at[u, chunk(ch)]

    def source(kind, layer, u, s):
        values = zown[s]
        xn = norm(2 + 2 * layer + kind, values)
        ln_n[u] = xn.astype(F32)

        def send_ln(ch, carry):
            rc(ln_n.at[u, chunk(ch)], ln_n.at[u, chunk(ch)], s_lnn.at[u, ch], r_lnn.at[u, ch], inward).start()
            return carry

        repeat(NCH, send_ln)
        ac_n[u] = values + kinds[kind](layer, xn)

        def send_ac(ch, carry):
            rc(ac_n.at[u, chunk(ch)], ac_n.at[u, chunk(ch)], s_acn.at[u, ch], r_acn.at[u, ch], inward).start()
            return carry

        repeat(NCH, send_ac)

    def sink(kind, layer, u, s):
        def wait_ln(ch, carry):
            rc(ln_f.at[u, chunk(ch)], ln_f.at[u, chunk(ch)], s_lnf.at[u, ch], r_lnf.at[u, ch], inward).wait_recv()
            return carry

        repeat(NCH, wait_ln)
        part = kinds[kind](layer, ln_f[u].astype(BF16))

        def wait_ac(ch, carry):
            rc(ac_f.at[u, chunk(ch)], ac_f.at[u, chunk(ch)], s_acf.at[u, ch], r_acf.at[u, ch], inward).wait_recv()
            return carry

        repeat(NCH, wait_ac)
        zown[s] = ac_f[u] + part

    def middle(kind, layer, u):
        def near_ln(ch, carry):
            rc(ln_n.at[u, chunk(ch)], ln_n.at[u, chunk(ch)], s_lnn.at[u, ch], r_lnn.at[u, ch], outward).wait_recv()
            rc(ln_n.at[u, chunk(ch)], ln_f.at[u, chunk(ch)], s_lnn.at[u, ch], r_lnf.at[u, ch], inward).start()
            return carry

        repeat(NCH, near_ln)
        zown[0] = kinds[kind](layer, ln_n[u].astype(BF16))

        def both(ch, carry):
            cp = rc(ln_f.at[u, chunk(ch)], ln_f.at[u, chunk(ch)], s_lnf.at[u, ch], r_lnf.at[u, ch], outward)
            cp.wait_recv()
            cp.start()
            rc(ac_n.at[u, chunk(ch)], ac_n.at[u, chunk(ch)], s_acn.at[u, ch], r_acn.at[u, ch], outward).wait_recv()
            ac_n[u, chunk(ch)] = ac_n[u, chunk(ch)] + zown[0, chunk(ch)]
            rc(ac_n.at[u, chunk(ch)], ac_f.at[u, chunk(ch)], s_acn.at[u, ch], r_acf.at[u, ch], inward).start()
            return carry

        repeat(NCH, both)
        zown[1] = kinds[kind](layer, ln_f[u].astype(BF16))
        if kind == 1:
            @pl.when(u == 7)
            def _():
                ag_relay(0, e_near, inward)

        def far_ac(ch, carry):
            cp = rc(ac_f.at[u, chunk(ch)], ac_f.at[u, chunk(ch)], s_acf.at[u, ch], r_acf.at[u, ch], outward)
            cp.wait_recv()
            ac_f[u, chunk(ch)] = ac_f[u, chunk(ch)] + zown[1, chunk(ch)]
            cp.start()
            return carry

        repeat(NCH, far_ac)

    def line_seq(i, e):
        return y * 8 + c * 4 + i * 2 + e

    def ag_copy(b, ch, sems, dev):
        return rc(zall.at[b, chunk(ch)], zall.at[b, chunk(ch)], sems.at[b, ch], r_ag.at[b, ch], dev)

    def ag_send(b, ch, z_dev):
        if z_dev is not None:
            ag_copy(b, ch, s_agz, z_dev).start()
        ag_copy(b, ch, s_agy, y_peer).start()
        ag_copy(b, ch, s_agc, core_peer).start()

    def ag_source(i):
        b = line_seq(i, e_near)
        zall[b] = norm(6, zown[i]).astype(F32)

        def step(ch, carry):
            ag_send(b, ch, inward)
            return carry

        repeat(NCH, step)

    def ag_relay(i, e, z_dev):
        b = line_seq(i, e)

        def step(ch, carry):
            ag_copy(b, ch, s_agz, inward).wait_recv()
            ag_send(b, ch, z_dev)
            return carry

        repeat(NCH, step)

    def ag_cross(i, e):
        b = (1 - y) * 8 + c * 4 + i * 2 + e

        def step(ch, carry):
            ag_copy(b, ch, s_agy, y_peer).wait_recv()
            ag_copy(b, ch, s_agc, core_peer).start()
            return carry

        repeat(NCH, step)

    for load in dec_loads:
        load.wait()

    def products(k, carry):
        part = pl.ds(pl.multiple_of(k * 256, 256), 256)
        wkq[part] = dot_t(emlp[0, part], wv[...]).astype(BF16)
        wvo[part] = dot(emlp[1, part], wo[...]).astype(BF16)
        return carry

    repeat(dim // 256, products)
    enc_loads = fetch(7, ((wkv_h.at[1], wv), (wo_h, wo), (emlp_h, emlp)))
    pair_step(1)
    for load in out_loads:
        load.wait()

    def out_products(k, carry):
        part = pl.ds(pl.multiple_of(k * 256, 256), 256)
        w2o[part] = dot(lw2[0, part], lw2[1]).astype(BF16)
        wvoo[part] = dot(wvo[part], lw2[1]).astype(BF16)
        return carry

    repeat(dim // 256, out_products)
    lat_loads = lat_loads + fetch(6, ((lw2_h, lw2),))
    w2o_copy = pltpu.make_async_copy(w2o, w2o_h, wsem.at[15])
    w2o_copy.start()
    def tail_loads():
        return [pltpu.make_async_copy(dmlp_h.at[0], emlp.at[0], wsem.at[10])]

    def order(k):
        i = lax.div(k, 8)
        r = lax.rem(k, 8)
        pair = lax.div(r, 2)
        odd = lax.rem(pair, 2)
        yb = y + odd - 2 * y * odd
        core = lax.rem(r, 2)
        cb = c + core - 2 * c * core
        far = lax.div(pair, 2)
        e = e_near + far - 2 * e_near * far
        return yb * 8 + cb * 4 + i * 2 + e

    def q_copy(k, par):
        return pltpu.make_async_copy(q_h.at[order(k)], (q0, q1)[par], qsem.at[par])

    def u_copy(k, par):
        return pltpu.make_async_copy((h0, h1)[par], out_h.at[order(k)], usem.at[par])

    def p_copy(k, par):
        return pltpu.make_async_copy((p0, p1)[par], p_h.at[order(k)], psem.at[par])

    def voo_copy(k, par):
        return pltpu.make_async_copy(voo_s.at[par], voo_h.at[order(k)], vsem.at[par])

    nrow = q0.shape[0]

    def decode_start():
        q_copy(0, 0).start()
        q_copy(1, 1).start()
        for load in tail_loads():
            load.wait()

    def prepare(k):
        zn = jnp.concatenate([zall[order(k)], zall[order(k + 1)]], axis=0).astype(BF16)

        def piece(weights, target):
            high, low = split_bf16(dot(zn, weights[...]))
            for j in range(2):
                target[j, 0:n, :] = high[j * n:(j + 1) * n]
                target[j, n:2 * n, :] = low[j * n:(j + 1) * n]

        return [functools.partial(piece, *pair) for pair in ((wkq, kq_s), (wvo, vo_s), (wvoo, voo_s))]

    parts = [slice(r, r + RBLK) for r in range(0, nrow, RBLK)]

    def norm_q(par):
        def piece(part):
            xq_s[part] = layer_norm((q0, q1)[par][part].astype(F32), nq_ref[0:1, :], nq_ref[1:2, :])

        return [functools.partial(piece, part) for part in parts]

    def score(par):
        def piece(part):
            both = dot_t(xq_s[part], kq_s[par])
            scores = (both + pltpu.roll(both, n, 1)) * (1.0 / math.sqrt(dim))
            weights = jnp.exp(scores - jnp.max(scores, axis=1, keepdims=True))
            (p0, p1)[par][part] = (weights / (0.5 * jnp.sum(weights, axis=1, keepdims=True))).astype(BF16)

        return [functools.partial(piece, part) for part in parts]

    def attend(par):
        def piece(part):
            (xu0, xu1)[par][part] = norm(7, dot((p0, p1)[par][part], vo_s[par]))

        return [functools.partial(piece, part) for part in parts]

    def expand(par):
        def piece(col):
            cols = slice(col, col + CBLK)
            (h0, h1)[par][:, cols] = gelu(dot((xu0, xu1)[par][...], emlp[0, :, cols])).astype(BF16)

        return [functools.partial(piece, col) for col in range(0, dim, CBLK)]

    def emit(*lists):
        for k in range(max(len(pieces) for pieces in lists)):
            for pieces in lists:
                if k < len(pieces):
                    pieces[k]()

    def decode_pair(kk, first):
        k = 2 * kk

        def step(ch, inner):
            ag_copy(order(k + 1), ch, s_agc, core_peer).wait_recv()
            return inner

        repeat(NCH, step)
        if not first:
            for par in range(2):
                voo_copy(k - 2 + par, par).wait()
            p_copy(k - 2, 0).wait()

            @pl.when(kk >= 2)
            def _():
                u_copy(k - 3, 1).wait()

        q_copy(k, 0).wait()
        emit(prepare(k), norm_q(0))
        emit([] if first else expand(1), score(0) + attend(0))
        for par in range(2):
            voo_copy(k + par, par).start()
        p_copy(k, 0).start()
        if not first:
            u_copy(k - 1, 1).start()

        @pl.when(kk < 7)
        def _():
            q_copy(k + 2, 0).start()

        q_copy(k + 1, 1).wait()
        if not first:
            u_copy(k - 2, 0).wait()
            p_copy(k - 1, 1).wait()
        emit(norm_q(1)[:1])
        emit(expand(0), norm_q(1)[1:] + score(1) + attend(1))
        p_copy(k + 1, 1).start()
        u_copy(k, 0).start()

        @pl.when(kk < 7)
        def _():
            q_copy(k + 3, 1).start()

    def decode_end():
        for par in range(2):
            voo_copy(14 + par, par).wait()
            p_copy(14 + par, par).wait()
        u_copy(13, 1).wait()
        emit(expand(1))
        u_copy(15, 1).start()
        u_copy(14, 0).wait()
        u_copy(15, 1).wait()
        w2o_copy.wait()

    def relays(kk):
        def far_relay(i):
            @pl.when(jnp.logical_and(is_mid, kk == (1, 3)[i]))
            def _():
                ag_relay(i, e_far, outward)

            @pl.when(jnp.logical_and(is_end, kk == (2, 5)[i]))
            def _():
                ag_relay(i, e_far, None)

        def near_relay(i):
            @pl.when(is_mid)
            def _():
                ag_relay(i, e_near, inward)

        pl.when(kk == 1)(lambda: ag_cross(0, e_near))
        far_relay(0)
        pl.when(kk == 2)(lambda: near_relay(1))
        pl.when(kk == 3)(lambda: ag_cross(0, e_far))
        far_relay(1)
        pl.when(kk == 4)(lambda: ag_cross(1, e_near))
        pl.when(kk == 6)(lambda: ag_cross(1, e_far))

    y_add(0)

    @pl.when(is_end)
    def _():
        z_end_send(0)

    @pl.when(is_mid)
    def _():
        z_mid(0)

    y_add(1)
    for load in lat_loads + enc_loads:
        load.wait()

    @pl.when(is_end)
    def _():
        z_end_send(1)

        def start(s, carry):
            both = jnp.concatenate(split_bf16(z_end_recv(s)), axis=0)
            both = dot(both, wv[...])
            attended = (both[0:n] + both[n:2 * n]).astype(BF16)
            z = lat_ref[...].astype(F32) + dot(attended, wo[...])
            zown[s] = z + dot(gelu(dot(norm(1, z), emlp[0])).astype(BF16), emlp[1])
            source(0, 0, s, s)
            return carry

        repeat(2, start)
        for load in tail_loads():
            load.start()

        def layer_step(layer, carry):
            def attn_unit(s, inner):
                u = layer * 4 + s
                sink(0, layer, u, s)
                source(1, layer, u + 2, s)
                return inner

            repeat(2, attn_unit)

            def mlp_unit(s, inner):
                u = layer * 4 + 2 + s

                @pl.when(u == 7)
                def _():
                    decode_start()
                    decode_pair(0, True)

                sink(1, layer, u, s)

                @pl.when(layer == 0)
                def _():
                    source(0, 1, u + 2, s)

                @pl.when(layer == 1)
                def _():
                    ag_source(s)

                return inner

            repeat(2, mlp_unit)
            return carry

        repeat(2, layer_step)

    @pl.when(is_mid)
    def _():
        z_mid(1)
        for load in tail_loads():
            load.start()

        def layer_step(layer, carry):
            for kind in range(2):
                def unit(s, inner):
                    middle(kind, layer, layer * 4 + 2 * kind + s)
                    return inner
                repeat(2, unit)
            return carry

        repeat(2, layer_step)

    @pl.when(is_mid)
    def _():
        decode_start()
        decode_pair(0, True)

    def tail_step(kk, carry):
        relays(kk)
        decode_pair(kk, False)
        return carry

    lax.fori_loop(1, 8, tail_step, 0)
    decode_end()

    def done_stats(p, carry):
        g, dev = peer(p)
        for i in range(2):
            stats_copy(i, me, g, dev).wait_send()
        return carry

    each_peer(done_stats)
    for i in range(2):
        core_copy(i, 1 - y).wait_send()
        core_copy(i, y).wait_send()
        for e in range(2):
            y_copy(i, e).wait_send()

    def done_z(i, carry):
        def step(ch, inner):
            rc(rz_a.at[i, chunk(ch)], rz_a.at[i, chunk(ch)], s_za.at[i, ch], r_za.at[i, ch], inward).wait_send()

            @pl.when(is_mid)
            def _():
                rc(rz_b.at[i, chunk(ch)], rz_b.at[i, chunk(ch)], s_zb.at[i, ch], r_zb.at[i, ch], outward).wait_send()

            return inner

        repeat(NCH, step)
        return carry

    repeat(2, done_z)

    def done_units(u, carry):
        def step(ch, inner):
            rc(ln_n.at[u, chunk(ch)], ln_n.at[u, chunk(ch)], s_lnn.at[u, ch], r_lnn.at[u, ch], inward).wait_send()
            rc(ac_n.at[u, chunk(ch)], ac_n.at[u, chunk(ch)], s_acn.at[u, ch], r_acn.at[u, ch], inward).wait_send()

            @pl.when(is_mid)
            def _():
                rc(ln_f.at[u, chunk(ch)], ln_f.at[u, chunk(ch)], s_lnf.at[u, ch], r_lnf.at[u, ch], outward).wait_send()
                rc(ac_f.at[u, chunk(ch)], ac_f.at[u, chunk(ch)], s_acf.at[u, ch], r_acf.at[u, ch], outward).wait_send()

            return inner

        repeat(NCH, step)
        return carry

    repeat(8, done_units)

    def done_ag(i, carry):
        for e in range(2):
            b = line_seq(i, e)
            other = (1 - y) * 8 + c * 4 + i * 2 + e

            def step(ch, inner):
                ag_copy(b, ch, s_agy, y_peer).wait_send()
                ag_copy(b, ch, s_agc, core_peer).wait_send()
                ag_copy(other, ch, s_agc, core_peer).wait_send()

                @pl.when(jnp.logical_or(is_mid, e == e_near))
                def _():
                    ag_copy(b, ch, s_agz, inward).wait_send()

                return inner

            repeat(NCH, step)
        return carry

    repeat(2, done_ag)


def latent_all(x_loc, q_loc, latents, norm_in, norm_lat, norm_query, enc_wq, enc_wkv, enc_wo, enc_mlp,
               wqkv, lwo, lw1, lw2, dec_wq, dec_wkv, dec_wo, dec_mlp, dec_out):
    nb, rows, dim = q_loc.shape
    n = latents.shape[0]
    vm = pl.BlockSpec(memory_space=pltpu.VMEM)
    hbm = pl.BlockSpec(memory_space=pl.ANY)
    dma = pltpu.SemaphoreType.DMA
    buf = lambda *shape: pltpu.VMEM(shape + (n, dim), F32)
    half = lambda *shape: pltpu.VMEM(shape + (dim,), BF16)
    return pl.pallas_call(
        latent_kernel,
        in_specs=[vm] * 4 + [hbm] * 15,
        out_specs=[hbm] * 4,
        out_shape=[jax.ShapeDtypeStruct(shape, BF16)
                   for shape in ((nb, rows, dim), (nb, rows, 2 * n), (nb, 2 * n, dim), (dim, dim))],
        scratch_shapes=[
            half(dim), half(dim), pltpu.VMEM(enc_mlp.shape, BF16),
            pltpu.VMEM(wqkv.shape, BF16), pltpu.VMEM(lwo.shape, BF16), pltpu.VMEM(lw1.shape, BF16), pltpu.VMEM(lw2.shape, BF16),
            dma((16,)), half(dim), half(dim), half(dim), half(dim),
            half(2, 2 * n), half(2, 2 * n), half(2, 2 * n), half(rows), half(rows), half(rows),
            pltpu.VMEM((rows, 2 * n), BF16), pltpu.VMEM((rows, 2 * n), BF16), half(rows), half(rows), half(rows), half(rows),
            half(4, rows), *[dma((2,))] * 5,
            buf(nb), half(2 * n), pltpu.VMEM((LANES, LANES), F32), pltpu.VMEM((2, nb, LANES), F32),
            pltpu.VMEM((2, 16, nb, LANES), F32), pltpu.VMEM((LANES, LANES), F32),
            buf(2, 2, 2), *[buf(2, 2)] * 3, *[buf(2)] * 2, *[buf(8)] * 4, buf(2), buf(nb),
            *[dma((2, 16))] * 2, *[dma((2, 2))] * 4, *[dma((2, NCH))] * 4,
        ] + [dma((8, NCH))] * 8 + [dma((nb, NCH))] * 4,
        compiler_params=pltpu.CompilerParams(vmem_limit_bytes=VMEM_LIMIT, collective_id=0, has_side_effects=True),
        name='latent_all',
    )(norm_in, latents, norm_lat, norm_query, x_loc, enc_wq, enc_wkv, enc_wo, enc_mlp, wqkv, lwo, lw1, lw2,
      q_loc, dec_wq, dec_wkv, dec_wo, dec_mlp, dec_out)


def out_kernel(h_ref, p_ref, voo_ref, w_ref, y_ref):
    for j in range(h_ref.shape[0]):
        y_ref[j] = dot(h_ref[j], w_ref[...]) + dot(p_ref[j], voo_ref[j])


def out_product(hidden, probs, voo, weights):
    nb, rows, dim = hidden.shape
    step = lambda *shape: pl.BlockSpec((OUT_STEP,) + shape, lambda b: (b, 0, 0))
    return pl.pallas_call(
        out_kernel,
        grid=(nb // OUT_STEP,),
        in_specs=[step(rows, dim), step(*probs.shape[1:]), step(*voo.shape[1:]), pl.BlockSpec((dim, dim), lambda b: (0, 0))],
        out_specs=step(rows, dim),
        out_shape=jax.ShapeDtypeStruct((nb, rows, dim), F32),
        compiler_params=pltpu.CompilerParams(vmem_limit_bytes=VMEM_LIMIT),
        name='out_product',
    )(hidden, probs, voo, weights)


def solution(mesh):
    seq_spec = P('dp', ('tp', 'sp'), None)
    replicated = P()
    in_specs = (seq_spec, seq_spec, replicated, replicated, replicated, replicated, replicated, replicated, replicated, replicated,
                P(None, None, None, 'tp', None), P(None, 'tp', None, None), P(None, None, 'tp'), P(None, 'tp', None),
                replicated, replicated, replicated, replicated, replicated)

    def device_step(x_loc, q_loc, latents, norm_in, norm_query, norm_lat, enc_wq, enc_wkv, enc_wo, enc_mlp,
                    lat_wqkv, lat_wo, lat_w1, lat_w2, dec_wq, dec_wkv, dec_wo, dec_mlp, dec_out):
        layers, dim = lat_wqkv.shape[0], latents.shape[1]
        wqkv = lat_wqkv.transpose(0, 2, 3, 1, 4)
        lwo = lat_wo.reshape(layers, -1, dim)
        parts = latent_all(x_loc, q_loc, latents, norm_in, norm_lat, norm_query, enc_wq, enc_wkv, enc_wo, enc_mlp,
                       wqkv, lwo, lat_w1, lat_w2, dec_wq, dec_wkv, dec_wo, dec_mlp, dec_out)
        return out_product(*parts)

    return jax.shard_map(device_step, mesh=mesh, in_specs=in_specs, out_specs=seq_spec, check_vma=False)
```

```python
import functools
import math
import jax
import jax.numpy as jnp
from jax import lax
from jax.experimental import pallas as pl
from jax.experimental.pallas import tpu as pltpu
from jax.sharding import PartitionSpec as P

LN_EPS = 1e-5
F32, BF16 = jnp.float32, jnp.bfloat16
MESH = pl.DeviceIdType.MESH
VMEM_LIMIT = 63 * 1024 * 1024
LANES = 128
NLINE = 4
RBLK = 128
CBLK = 256
OUT_STEP = 4
PAIR_AT = 4
NCH = 4
GELU_C = math.sqrt(2.0 / math.pi)


def layer_norm(values, gain, bias):
    row_mean = jnp.mean(values, axis=-1, keepdims=True)
    centered = values - row_mean
    row_var = jnp.mean(centered * centered, axis=-1, keepdims=True)
    return (centered * lax.rsqrt(row_var + LN_EPS) * gain + bias).astype(BF16)


def gelu(x):
    return 0.5 * x * (1.0 + jnp.tanh(GELU_C * (x + 0.044715 * (x * x * x))))


def repeat(count, step):
    lax.fori_loop(0, count, step, 0)


def each_peer(step):
    lax.fori_loop(1, 16, step, 0)


def dot(a, b):
    return jnp.dot(a, b, preferred_element_type=F32)


def dot_t(a, b):
    return lax.dot_general(a, b, (((1,), (1,)), ((), ())), preferred_element_type=F32)


def split_bf16(x):
    high = x.astype(BF16)
    return high, (x - high.astype(F32)).astype(BF16)


def latent_kernel(nin_ref, lat_ref, nlat_ref, nq_ref, x_h, ewq_h, wkv_h, wo_h, emlp_h, qkv_h, lwo_h, lw1_h, lw2_h,
                  q_h, dwq_h, dwkv_h, dwo_h, dmlp_h, dout_h, out_h, p_h, voo_h, w2o_h,
                  wv, wo, emlp, wqkv, lwo, lw1, lw2, wsem, wkq, wvo, wvoo, w2o,
                  kq_s, vo_s, voo_s, xq_s, xu0, xu1, p0, p1, q0, q1, h0, h1, xbuf, qsem, usem, psem, vsem, xsem,
                  num, qk_s, stats_s, st_mine,
                  st_all, gs, d2d, ysend, yrecv, zsum, rz_a, rz_b, ln_n, ln_f, ac_n, ac_f, zown, zall,
                  s_st, r_st, s_d2, r_d2, s_y, r_y, s_za, s_zb, r_za, r_zb,
                  s_lnn, s_lnf, s_acn, s_acf, r_lnn, r_lnf, r_acn, r_acf, r_ag, s_agz, s_agc, s_agy):
    n, dim = lat_ref.shape
    rows = n // NCH
    x = lax.axis_index('dp')
    t = lax.axis_index('tp')
    sp = lax.axis_index('sp')
    y = lax.div(sp, 2)
    c = lax.rem(sp, 2)
    me = t * 4 + sp
    upper = lax.div(t, 2)
    is_end = jnp.logical_or(t == 0, t == NLINE - 1)
    is_mid = jnp.logical_not(is_end)
    e_near = upper
    e_far = 1 - upper
    inward = (x, jnp.where(t == 0, 1, jnp.where(t == 1, 2, jnp.where(t == 2, 1, 2))), sp)
    outward = (x, jnp.where(t <= 1, 0, NLINE - 1), sp)
    core_peer = (x, t, y * 2 + (1 - c))
    y_peer = (x, t, (1 - y) * 2 + c)

    def rc(src, dst, ssem, rsem, dev):
        return pltpu.make_async_remote_copy(src_ref=src, dst_ref=dst, send_sem=ssem, recv_sem=rsem,
                                            device_id=dev, device_id_type=MESH)

    def peer(p):
        g = lax.rem(me + p, 16)
        return g, (x, lax.div(g, 4), lax.rem(g, 4))

    def fetch(first, pairs):
        copies = [pltpu.make_async_copy(src, dst, wsem.at[first + k]) for k, (src, dst) in enumerate(pairs)]
        for copy in copies:
            copy.start()
        return copies

    def x_copy(g):
        first, _, _ = group(g)
        slot = lax.rem(g, 2)
        return pltpu.make_async_copy(x_h.at[pl.ds(first, 2)], xbuf.at[pl.ds(2 * slot, 2)], xsem.at[slot])

    def group(g):
        i = lax.div(g, 4)
        j = lax.rem(g, 4)
        core = lax.div(j, 2)
        cb = 1 - c + core * (2 * c - 1)
        side = lax.rem(j, 2)
        yb = 1 - y + side * (2 * y - 1)
        return yb * 8 + cb * 4 + i * 2, i, j

    query_loads = fetch(0, ((ewq_h, wv), (wkv_h.at[0], wo)))
    x_copy(0).start()
    key_loads = fetch(2, ((dwkv_h, emlp),))
    lat_loads = fetch(3, ((qkv_h, wqkv), (lwo_h, lwo), (lw1_h, lw1)))
    out_loads = fetch(13, ((dmlp_h.at[1], lw2.at[0]), (dout_h, lw2.at[1])))

    barrier = pltpu.get_barrier_semaphore()

    def greet(p, carry):
        pl.semaphore_signal(barrier, inc=1, device_id=peer(p)[1], device_id_type=MESH)
        return carry

    each_peer(greet)

    def norm(index, values):
        return layer_norm(values, nlat_ref[index, 0:1, :], nlat_ref[index, 1:2, :])

    for load in query_loads:
        load.wait()
    q = dot(norm(0, lat_ref[...].astype(F32)), wv[...]).astype(BF16)
    high, low = split_bf16(dot_t(q, wo[...]))
    qk_s[0:n, :] = high
    qk_s[n:2 * n, :] = low
    stats_s[...] = jnp.zeros_like(stats_s)
    dec_loads = key_loads + fetch(11, ((dwq_h, wv), (dwo_h, wo)))

    def core_copy(i, yb):
        return rc(num.at[pl.ds(yb * 8 + (1 - c) * 4 + i * 2, 2)], d2d.at[i, yb], s_d2.at[i, yb], r_d2.at[i, yb], core_peer)

    def y_copy(i, e):
        return rc(ysend.at[i, e], yrecv.at[i, e], s_y.at[i, e], r_y.at[i, e], y_peer)

    def stats_copy(i, src, g, dev):
        return rc(st_mine.at[i], st_all.at[i, src], s_st.at[i, g], r_st.at[i, src], dev)

    lane = lax.broadcasted_iota(jnp.int32, (2 * n, LANES), 1)

    partner = t * 4 + y * 2 + (1 - c)

    def set_scales(first, second):
        gs[...] = jnp.zeros_like(gs)
        gs[0:16, :] = first
        upper_part = gs[...].T[0:n, :]
        gs[0:16, :] = second
        lower_part = gs[...].T[0:n, :]
        gs[0:n, :] = upper_part
        gs[n:2 * n, :] = lower_part

    def scales(b):
        col = jnp.sum(jnp.where(lane == b, gs[...], 0.0), axis=1, keepdims=True)
        return col[0:n], col[n:2 * n]

    def pair_step(i):
        stats_copy(i, partner, partner, core_peer).wait_recv()
        mine, other = st_all[i, me], st_all[i, partner]
        top = jnp.maximum(mine, other)
        set_scales(jnp.exp(mine - top), jnp.exp(other - top))
        for side in range(2):
            yb = y if side else 1 - y
            core_copy(i, yb).wait_recv()
            for e in range(2):
                b = yb * 8 + c * 4 + i * 2 + e
                first, second = scales(b)
                value = first * num[b] + second * d2d[i, yb, e]
                if side:
                    zsum[i, e] = value
                else:
                    ysend[i, e] = value
                    y_copy(i, e).start()

    def encode(g, carry):
        first, i, j = group(g)
        x_copy(g).wait()

        @pl.when(g < 7)
        def _():
            x_copy(g + 1).start()

        slot = 2 * lax.rem(g, 2)
        each = range(2)
        xns = [layer_norm(xbuf[slot + k].astype(F32), nin_ref[0:1, :], nin_ref[1:2, :]) for k in each]
        both = [dot_t(qk_s[...], xn) for xn in xns]
        scores = [(v[:n] + v[n:]) * (1.0 / math.sqrt(dim)) for v in both]
        maxima = [jnp.max(v, axis=1, keepdims=True) for v in scores]
        weights = [jnp.exp(v - m) for v, m in zip(scores, maxima)]
        sums = [jnp.sum(v, axis=1, keepdims=True) for v in weights]
        for k in each:
            num[first + k] = dot(weights[k].astype(BF16), xns[k])
            here = lax.broadcasted_iota(jnp.int32, (n, LANES), 1) == first + k
            stats_s[0:n, :] = jnp.where(here, maxima[k], stats_s[0:n, :])
            stats_s[n:2 * n, :] = jnp.where(here, sums[k], stats_s[n:2 * n, :])

        @pl.when(j == 1)
        def _():
            core_copy(i, 1 - y).start()
            core_copy(i, y).start()

        @pl.when(j == 3)
        def _():
            mine = stats_s[...].T[0:16, :]
            st_mine[i] = mine
            st_all[i, me] = mine

            def send_stats(p, inner):
                dst, dev = peer(p)
                stats_copy(i, me, dst, dev).start()
                return inner

            each_peer(send_stats)

        @pl.when(g == PAIR_AT)
        def _():
            pair_step(0)

        return carry

    pl.semaphore_wait(barrier, 15)
    repeat(8, encode)

    def y_add(i):
        def wait_stats(p, carry):
            g, dev = peer(p)

            @pl.when(g != partner)
            def _():
                stats_copy(i, g, g, dev).wait_recv()

            return carry

        each_peer(wait_stats)
        top = lax.fori_loop(1, 16, lambda d, m: jnp.maximum(m, st_all[i, d]), st_all[i, 0])

        def add_sum(d, total):
            stats = st_all[i, d]
            return total + jnp.exp(stats - top) * pltpu.roll(stats, n, 1)

        total = lax.fori_loop(0, 16, add_sum, jnp.zeros_like(top))
        across = t * 4 + (1 - y) * 2
        here = jnp.maximum(st_all[i, me], st_all[i, partner])
        there = jnp.maximum(st_all[i, across], st_all[i, across + 1])
        set_scales(jnp.exp(here - top) / total, jnp.exp(there - top) / total)
        for e in range(2):
            first, second = scales(y * 8 + c * 4 + i * 2 + e)
            y_copy(i, e).wait_recv()
            zsum[i, e] = first * zsum[i, e] + second * yrecv[i, e]

    def chunk(ch):
        return pl.ds(pl.multiple_of(ch * rows, rows), rows)

    def z_end_send(i):
        def step(ch, carry):
            rc(zsum.at[i, e_far, chunk(ch)], rz_a.at[i, chunk(ch)], s_za.at[i, ch], r_za.at[i, ch], inward).start()
            return carry
        repeat(NCH, step)

    def z_mid(i):
        def near(ch, carry):
            cp = rc(rz_a.at[i, chunk(ch)], rz_b.at[i, chunk(ch)], s_za.at[i, ch], r_zb.at[i, ch], inward)
            rc(rz_a.at[i, chunk(ch)], rz_a.at[i, chunk(ch)], s_za.at[i, ch], r_za.at[i, ch], outward).wait_recv()
            rz_a[i, chunk(ch)] = rz_a[i, chunk(ch)] + zsum[i, e_far, chunk(ch)]
            cp.start()
            return carry

        def far(ch, carry):
            cp = rc(rz_b.at[i, chunk(ch)], rz_b.at[i, chunk(ch)], s_zb.at[i, ch], r_zb.at[i, ch], outward)
            cp.wait_recv()
            rz_b[i, chunk(ch)] = rz_b[i, chunk(ch)] + zsum[i, e_near, chunk(ch)]
            cp.start()
            return carry

        repeat(NCH, near)
        repeat(NCH, far)

    def z_end_recv(i):
        def step(ch, carry):
            rc(rz_b.at[i, chunk(ch)], rz_b.at[i, chunk(ch)], s_zb.at[i, ch], r_zb.at[i, ch], inward).wait_recv()
            return carry
        repeat(NCH, step)
        return rz_b[i] + zsum[i, e_near]

    def attention(layer, xn):
        hd = wqkv.shape[4]
        qkv = [dot(xn, jnp.concatenate([wqkv[layer, j, 0], wqkv[layer, j, 1]], axis=1)).astype(BF16) for j in range(3)]
        outs = []
        for h in range(2):
            q, k, v = (part[:, h * hd:(h + 1) * hd] for part in qkv)
            scores = dot_t(q, k) * (1.0 / math.sqrt(hd))
            weights = jnp.exp(scores - jnp.max(scores, axis=1, keepdims=True))
            probs = (weights / jnp.sum(weights, axis=1, keepdims=True)).astype(BF16)
            outs.append(dot(probs, v).astype(BF16))
        return dot(jnp.concatenate(outs, axis=1), lwo[layer])

    def mlp(layer, xn):
        return dot(gelu(dot(xn, lw1[layer])).astype(BF16), lw2[layer])

    kinds = (attention, mlp)

    def ln_near(u, ch):
        return ln_n.at[u, chunk(ch)]

    def source(kind, layer, u, s):
        values = zown[s]
        xn = norm(2 + 2 * layer + kind, values)
        ln_n[u] = xn.astype(F32)

        def send_ln(ch, carry):
            rc(ln_n.at[u, chunk(ch)], ln_n.at[u, chunk(ch)], s_lnn.at[u, ch], r_lnn.at[u, ch], inward).start()
            return carry

        repeat(NCH, send_ln)
        ac_n[u] = values + kinds[kind](layer, xn)

        def send_ac(ch, carry):
            rc(ac_n.at[u, chunk(ch)], ac_n.at[u, chunk(ch)], s_acn.at[u, ch], r_acn.at[u, ch], inward).start()
            return carry

        repeat(NCH, send_ac)

    def sink(kind, layer, u, s):
        def wait_ln(ch, carry):
            rc(ln_f.at[u, chunk(ch)], ln_f.at[u, chunk(ch)], s_lnf.at[u, ch], r_lnf.at[u, ch], inward).wait_recv()
            return carry

        repeat(NCH, wait_ln)
        part = kinds[kind](layer, ln_f[u].astype(BF16))

        def wait_ac(ch, carry):
            rc(ac_f.at[u, chunk(ch)], ac_f.at[u, chunk(ch)], s_acf.at[u, ch], r_acf.at[u, ch], inward).wait_recv()
            return carry

        repeat(NCH, wait_ac)
        zown[s] = ac_f[u] + part

    def middle(kind, layer, u):
        def near_ln(ch, carry):
            rc(ln_n.at[u, chunk(ch)], ln_n.at[u, chunk(ch)], s_lnn.at[u, ch], r_lnn.at[u, ch], outward).wait_recv()
            rc(ln_n.at[u, chunk(ch)], ln_f.at[u, chunk(ch)], s_lnn.at[u, ch], r_lnf.at[u, ch], inward).start()
            return carry

        repeat(NCH, near_ln)
        zown[0] = kinds[kind](layer, ln_n[u].astype(BF16))

        def both(ch, carry):
            cp = rc(ln_f.at[u, chunk(ch)], ln_f.at[u, chunk(ch)], s_lnf.at[u, ch], r_lnf.at[u, ch], outward)
            cp.wait_recv()
            cp.start()
            rc(ac_n.at[u, chunk(ch)], ac_n.at[u, chunk(ch)], s_acn.at[u, ch], r_acn.at[u, ch], outward).wait_recv()
            ac_n[u, chunk(ch)] = ac_n[u, chunk(ch)] + zown[0, chunk(ch)]
            rc(ac_n.at[u, chunk(ch)], ac_f.at[u, chunk(ch)], s_acn.at[u, ch], r_acf.at[u, ch], inward).start()
            return carry

        repeat(NCH, both)
        zown[1] = kinds[kind](layer, ln_f[u].astype(BF16))
        if kind == 1:
            @pl.when(u == 7)
            def _():
                ag_relay(0, e_near, inward)

        def far_ac(ch, carry):
            cp = rc(ac_f.at[u, chunk(ch)], ac_f.at[u, chunk(ch)], s_acf.at[u, ch], r_acf.at[u, ch], outward)
            cp.wait_recv()
            ac_f[u, chunk(ch)] = ac_f[u, chunk(ch)] + zown[1, chunk(ch)]
            cp.start()
            return carry

        repeat(NCH, far_ac)

    def line_seq(i, e):
        return y * 8 + c * 4 + i * 2 + e

    def ag_copy(b, ch, sems, dev):
        return rc(zall.at[b, chunk(ch)], zall.at[b, chunk(ch)], sems.at[b, ch], r_ag.at[b, ch], dev)

    def ag_send(b, ch, z_dev):
        if z_dev is not None:
            ag_copy(b, ch, s_agz, z_dev).start()
        ag_copy(b, ch, s_agy, y_peer).start()
        ag_copy(b, ch, s_agc, core_peer).start()

    def ag_source(i):
        b = line_seq(i, e_near)
        zall[b] = norm(6, zown[i]).astype(F32)

        def step(ch, carry):
            ag_send(b, ch, inward)
            return carry

        repeat(NCH, step)

    def ag_relay(i, e, z_dev):
        b = line_seq(i, e)

        def step(ch, carry):
            ag_copy(b, ch, s_agz, inward).wait_recv()
            ag_send(b, ch, z_dev)
            return carry

        repeat(NCH, step)

    def ag_cross(i, e):
        b = (1 - y) * 8 + c * 4 + i * 2 + e

        def step(ch, carry):
            ag_copy(b, ch, s_agy, y_peer).wait_recv()
            ag_copy(b, ch, s_agc, core_peer).start()
            return carry

        repeat(NCH, step)

    for load in dec_loads:
        load.wait()

    def products(k, carry):
        part = pl.ds(pl.multiple_of(k * 256, 256), 256)
        wkq[part] = dot_t(emlp[0, part], wv[...]).astype(BF16)
        wvo[part] = dot(emlp[1, part], wo[...]).astype(BF16)
        return carry

    repeat(dim // 256, products)
    enc_loads = fetch(7, ((wkv_h.at[1], wv), (wo_h, wo), (emlp_h, emlp)))
    pair_step(1)
    for load in out_loads:
        load.wait()

    def out_products(k, carry):
        part = pl.ds(pl.multiple_of(k * 256, 256), 256)
        w2o[part] = dot(lw2[0, part], lw2[1]).astype(BF16)
        wvoo[part] = dot(wvo[part], lw2[1]).astype(BF16)
        return carry

    halfway = dim // 512
    repeat(halfway, out_products)
    def tail_loads():
        return [pltpu.make_async_copy(dmlp_h.at[0], emlp.at[0], wsem.at[10])]

    def order(k):
        i = lax.div(k, 8)
        r = lax.rem(k, 8)
        pair = lax.div(r, 2)
        odd = lax.rem(pair, 2)
        yb = y + odd - 2 * y * odd
        core = lax.rem(r, 2)
        cb = c + core - 2 * c * core
        far = lax.div(pair, 2)
        e = e_near + far - 2 * e_near * far
        return yb * 8 + cb * 4 + i * 2 + e

    def q_copy(k, par):
        return pltpu.make_async_copy(q_h.at[order(k)], (q0, q1)[par], qsem.at[par])

    def u_copy(k, par):
        return pltpu.make_async_copy((h0, h1)[par], out_h.at[order(k)], usem.at[par])

    def p_copy(k, par):
        return pltpu.make_async_copy((p0, p1)[par], p_h.at[order(k)], psem.at[par])

    def voo_copy(k, par):
        return pltpu.make_async_copy(voo_s.at[par], voo_h.at[order(k)], vsem.at[par])

    nrow = q0.shape[0]

    def decode_start():
        q_copy(0, 0).start()
        q_copy(1, 1).start()
        for load in tail_loads():
            load.wait()

    def prepare(k):
        zn = jnp.concatenate([zall[order(k)], zall[order(k + 1)]], axis=0).astype(BF16)

        def piece(weights, target):
            high, low = split_bf16(dot(zn, weights[...]))
            for j in range(2):
                target[j, 0:n, :] = high[j * n:(j + 1) * n]
                target[j, n:2 * n, :] = low[j * n:(j + 1) * n]

        return [functools.partial(piece, *pair) for pair in ((wkq, kq_s), (wvo, vo_s), (wvoo, voo_s))]

    parts = [slice(r, r + RBLK) for r in range(0, nrow, RBLK)]

    def norm_q(par):
        def piece(part):
            xq_s[part] = layer_norm((q0, q1)[par][part].astype(F32), nq_ref[0:1, :], nq_ref[1:2, :])

        return [functools.partial(piece, part) for part in parts]

    def score(par):
        def piece(part):
            both = dot_t(xq_s[part], kq_s[par])
            scores = (both + pltpu.roll(both, n, 1)) * (1.0 / math.sqrt(dim))
            weights = jnp.exp(scores - jnp.max(scores, axis=1, keepdims=True))
            (p0, p1)[par][part] = (weights / (0.5 * jnp.sum(weights, axis=1, keepdims=True))).astype(BF16)

        return [functools.partial(piece, part) for part in parts]

    def attend(par):
        def piece(part):
            (xu0, xu1)[par][part] = norm(7, dot((p0, p1)[par][part], vo_s[par]))

        return [functools.partial(piece, part) for part in parts]

    def expand(par):
        def piece(col):
            cols = slice(col, col + CBLK)
            (h0, h1)[par][:, cols] = gelu(dot((xu0, xu1)[par][...], emlp[0, :, cols])).astype(BF16)

        return [functools.partial(piece, col) for col in range(0, dim, CBLK)]

    def emit(*lists):
        for k in range(max(len(pieces) for pieces in lists)):
            for pieces in lists:
                if k < len(pieces):
                    pieces[k]()

    def decode_pair(kk, first):
        k = 2 * kk

        def step(ch, inner):
            ag_copy(order(k + 1), ch, s_agc, core_peer).wait_recv()
            return inner

        repeat(NCH, step)
        if not first:
            for par in range(2):
                voo_copy(k - 2 + par, par).wait()
            p_copy(k - 2, 0).wait()

            @pl.when(kk >= 2)
            def _():
                u_copy(k - 3, 1).wait()

        q_copy(k, 0).wait()
        emit(prepare(k), norm_q(0))
        emit([] if first else expand(1), score(0) + attend(0))
        for par in range(2):
            voo_copy(k + par, par).start()
        p_copy(k, 0).start()
        if not first:
            u_copy(k - 1, 1).start()

        @pl.when(kk < 7)
        def _():
            q_copy(k + 2, 0).start()

        q_copy(k + 1, 1).wait()
        if not first:
            u_copy(k - 2, 0).wait()
            p_copy(k - 1, 1).wait()
        emit(norm_q(1)[:1])
        emit(expand(0), norm_q(1)[1:] + score(1) + attend(1))
        p_copy(k + 1, 1).start()
        u_copy(k, 0).start()

        @pl.when(kk < 7)
        def _():
            q_copy(k + 3, 1).start()

    def decode_end():
        for par in range(2):
            voo_copy(14 + par, par).wait()
            p_copy(14 + par, par).wait()
        u_copy(13, 1).wait()
        emit(expand(1))
        u_copy(15, 1).start()
        u_copy(14, 0).wait()
        u_copy(15, 1).wait()
        w2o_copy.wait()

    def relays(kk):
        def far_relay(i):
            @pl.when(jnp.logical_and(is_mid, kk == (1, 3)[i]))
            def _():
                ag_relay(i, e_far, outward)

            @pl.when(jnp.logical_and(is_end, kk == (2, 5)[i]))
            def _():
                ag_relay(i, e_far, None)

        def near_relay(i):
            @pl.when(is_mid)
            def _():
                ag_relay(i, e_near, inward)

        pl.when(kk == 1)(lambda: ag_cross(0, e_near))
        far_relay(0)
        pl.when(kk == 2)(lambda: near_relay(1))
        pl.when(kk == 3)(lambda: ag_cross(0, e_far))
        far_relay(1)
        pl.when(kk == 4)(lambda: ag_cross(1, e_near))
        pl.when(kk == 6)(lambda: ag_cross(1, e_far))

    y_add(0)

    @pl.when(is_end)
    def _():
        z_end_send(0)

    lax.fori_loop(halfway, 2 * halfway, out_products, 0)
    lat_loads = lat_loads + fetch(6, ((lw2_h, lw2),))
    w2o_copy = pltpu.make_async_copy(w2o, w2o_h, wsem.at[15])
    w2o_copy.start()

    @pl.when(is_mid)
    def _():
        z_mid(0)

    y_add(1)
    for load in lat_loads + enc_loads:
        load.wait()

    @pl.when(is_end)
    def _():
        z_end_send(1)

        def start(s, carry):
            both = jnp.concatenate(split_bf16(z_end_recv(s)), axis=0)
            both = dot(both, wv[...])
            attended = (both[0:n] + both[n:2 * n]).astype(BF16)
            z = lat_ref[...].astype(F32) + dot(attended, wo[...])
            zown[s] = z + dot(gelu(dot(norm(1, z), emlp[0])).astype(BF16), emlp[1])
            source(0, 0, s, s)
            return carry

        repeat(2, start)
        for load in tail_loads():
            load.start()

        def layer_step(layer, carry):
            def attn_unit(s, inner):
                u = layer * 4 + s
                sink(0, layer, u, s)
                source(1, layer, u + 2, s)
                return inner

            repeat(2, attn_unit)

            def mlp_unit(s, inner):
                u = layer * 4 + 2 + s

                @pl.when(u == 7)
                def _():
                    decode_start()
                    decode_pair(0, True)

                sink(1, layer, u, s)

                @pl.when(layer == 0)
                def _():
                    source(0, 1, u + 2, s)

                @pl.when(layer == 1)
                def _():
                    ag_source(s)

                return inner

            repeat(2, mlp_unit)
            return carry

        repeat(2, layer_step)

    @pl.when(is_mid)
    def _():
        z_mid(1)
        for load in tail_loads():
            load.start()

        def layer_step(layer, carry):
            for kind in range(2):
                def unit(s, inner):
                    middle(kind, layer, layer * 4 + 2 * kind + s)
                    return inner
                repeat(2, unit)
            return carry

        repeat(2, layer_step)

    @pl.when(is_mid)
    def _():
        decode_start()
        decode_pair(0, True)

    def tail_step(kk, carry):
        relays(kk)
        decode_pair(kk, False)
        return carry

    lax.fori_loop(1, 8, tail_step, 0)
    decode_end()

    def done_stats(p, carry):
        g, dev = peer(p)
        for i in range(2):
            stats_copy(i, me, g, dev).wait_send()
        return carry

    each_peer(done_stats)
    for i in range(2):
        core_copy(i, 1 - y).wait_send()
        core_copy(i, y).wait_send()
        for e in range(2):
            y_copy(i, e).wait_send()

    def done_z(i, carry):
        def step(ch, inner):
            rc(rz_a.at[i, chunk(ch)], rz_a.at[i, chunk(ch)], s_za.at[i, ch], r_za.at[i, ch], inward).wait_send()

            @pl.when(is_mid)
            def _():
                rc(rz_b.at[i, chunk(ch)], rz_b.at[i, chunk(ch)], s_zb.at[i, ch], r_zb.at[i, ch], outward).wait_send()

            return inner

        repeat(NCH, step)
        return carry

    repeat(2, done_z)

    def done_units(u, carry):
        def step(ch, inner):
            rc(ln_n.at[u, chunk(ch)], ln_n.at[u, chunk(ch)], s_lnn.at[u, ch], r_lnn.at[u, ch], inward).wait_send()
            rc(ac_n.at[u, chunk(ch)], ac_n.at[u, chunk(ch)], s_acn.at[u, ch], r_acn.at[u, ch], inward).wait_send()

            @pl.when(is_mid)
            def _():
                rc(ln_f.at[u, chunk(ch)], ln_f.at[u, chunk(ch)], s_lnf.at[u, ch], r_lnf.at[u, ch], outward).wait_send()
                rc(ac_f.at[u, chunk(ch)], ac_f.at[u, chunk(ch)], s_acf.at[u, ch], r_acf.at[u, ch], outward).wait_send()

            return inner

        repeat(NCH, step)
        return carry

    repeat(8, done_units)

    def done_ag(i, carry):
        for e in range(2):
            b = line_seq(i, e)
            other = (1 - y) * 8 + c * 4 + i * 2 + e

            def step(ch, inner):
                ag_copy(b, ch, s_agy, y_peer).wait_send()
                ag_copy(b, ch, s_agc, core_peer).wait_send()
                ag_copy(other, ch, s_agc, core_peer).wait_send()

                @pl.when(jnp.logical_or(is_mid, e == e_near))
                def _():
                    ag_copy(b, ch, s_agz, inward).wait_send()

                return inner

            repeat(NCH, step)
        return carry

    repeat(2, done_ag)


def latent_all(x_loc, q_loc, latents, norm_in, norm_lat, norm_query, enc_wq, enc_wkv, enc_wo, enc_mlp,
               wqkv, lwo, lw1, lw2, dec_wq, dec_wkv, dec_wo, dec_mlp, dec_out):
    nb, rows, dim = q_loc.shape
    n = latents.shape[0]
    vm = pl.BlockSpec(memory_space=pltpu.VMEM)
    hbm = pl.BlockSpec(memory_space=pl.ANY)
    dma = pltpu.SemaphoreType.DMA
    buf = lambda *shape: pltpu.VMEM(shape + (n, dim), F32)
    half = lambda *shape: pltpu.VMEM(shape + (dim,), BF16)
    return pl.pallas_call(
        latent_kernel,
        in_specs=[vm] * 4 + [hbm] * 15,
        out_specs=[hbm] * 4,
        out_shape=[jax.ShapeDtypeStruct(shape, BF16)
                   for shape in ((nb, rows, dim), (nb, rows, 2 * n), (nb, 2 * n, dim), (dim, dim))],
        scratch_shapes=[
            half(dim), half(dim), pltpu.VMEM(enc_mlp.shape, BF16),
            pltpu.VMEM(wqkv.shape, BF16), pltpu.VMEM(lwo.shape, BF16), pltpu.VMEM(lw1.shape, BF16), pltpu.VMEM(lw2.shape, BF16),
            dma((16,)), half(dim), half(dim), half(dim), half(dim),
            half(2, 2 * n), half(2, 2 * n), half(2, 2 * n), half(rows), half(rows), half(rows),
            pltpu.VMEM((rows, 2 * n), BF16), pltpu.VMEM((rows, 2 * n), BF16), half(rows), half(rows), half(rows), half(rows),
            half(4, rows), *[dma((2,))] * 5,
            buf(nb), half(2 * n), pltpu.VMEM((LANES, LANES), F32), pltpu.VMEM((2, nb, LANES), F32),
            pltpu.VMEM((2, 16, nb, LANES), F32), pltpu.VMEM((LANES, LANES), F32),
            buf(2, 2, 2), *[buf(2, 2)] * 3, *[buf(2)] * 2, *[buf(8)] * 4, buf(2), buf(nb),
            *[dma((2, 16))] * 2, *[dma((2, 2))] * 4, *[dma((2, NCH))] * 4,
        ] + [dma((8, NCH))] * 8 + [dma((nb, NCH))] * 4,
        compiler_params=pltpu.CompilerParams(vmem_limit_bytes=VMEM_LIMIT, collective_id=0, has_side_effects=True),
        name='latent_all',
    )(norm_in, latents, norm_lat, norm_query, x_loc, enc_wq, enc_wkv, enc_wo, enc_mlp, wqkv, lwo, lw1, lw2,
      q_loc, dec_wq, dec_wkv, dec_wo, dec_mlp, dec_out)


def out_kernel(h_ref, p_ref, voo_ref, w_ref, y_ref):
    for j in range(h_ref.shape[0]):
        y_ref[j] = dot(h_ref[j], w_ref[...]) + dot(p_ref[j], voo_ref[j])


def out_product(hidden, probs, voo, weights):
    nb, rows, dim = hidden.shape
    step = lambda *shape: pl.BlockSpec((OUT_STEP,) + shape, lambda b: (b, 0, 0))
    return pl.pallas_call(
        out_kernel,
        grid=(nb // OUT_STEP,),
        in_specs=[step(rows, dim), step(*probs.shape[1:]), step(*voo.shape[1:]), pl.BlockSpec((dim, dim), lambda b: (0, 0))],
        out_specs=step(rows, dim),
        out_shape=jax.ShapeDtypeStruct((nb, rows, dim), F32),
        compiler_params=pltpu.CompilerParams(vmem_limit_bytes=VMEM_LIMIT),
        name='out_product',
    )(hidden, probs, voo, weights)


def solution(mesh):
    seq_spec = P('dp', ('tp', 'sp'), None)
    replicated = P()
    in_specs = (seq_spec, seq_spec, replicated, replicated, replicated, replicated, replicated, replicated, replicated, replicated,
                P(None, None, None, 'tp', None), P(None, 'tp', None, None), P(None, None, 'tp'), P(None, 'tp', None),
                replicated, replicated, replicated, replicated, replicated)

    def device_step(x_loc, q_loc, latents, norm_in, norm_query, norm_lat, enc_wq, enc_wkv, enc_wo, enc_mlp,
                    lat_wqkv, lat_wo, lat_w1, lat_w2, dec_wq, dec_wkv, dec_wo, dec_mlp, dec_out):
        layers, dim = lat_wqkv.shape[0], latents.shape[1]
        wqkv = lat_wqkv.transpose(0, 2, 3, 1, 4)
        lwo = lat_wo.reshape(layers, -1, dim)
        parts = latent_all(x_loc, q_loc, latents, norm_in, norm_lat, norm_query, enc_wq, enc_wkv, enc_wo, enc_mlp,
                       wqkv, lwo, lat_w1, lat_w2, dec_wq, dec_wkv, dec_wo, dec_mlp, dec_out)
        return out_product(*parts)

    return jax.shard_map(device_step, mesh=mesh, in_specs=in_specs, out_specs=seq_spec, check_vma=False)
```
